32 devices in a mesh: gx: 8 (over z, y), gy: 4 (over x, core).
Axes of the slice: x: 2, y: 2, z: 4, core: 2. Of those that a mesh axis runs over, the one named last changes fastest.
Arguments:
- level_cotangent: float32 [128, 64, 128], P('gx', 'gy'), may hold values from -6 to 6
- velocity_cotangent: float32 [3, 128, 64, 128], P(None, 'gx', 'gy'), may hold values from -6 to 6
- fraction: float32 [2, 3, 128, 64, 128], P(None, None, 'gx', 'gy'), may hold values from 0 to 1
- shift_x: int32 [8, 4, 2], P('gx', 'gy'), may hold values from -2 to 2
- shift_y: int32 [8, 4, 2], P('gx', 'gy'), may hold values from -1 to 1
- region_labels: int32 [128, 64, 128], P('gx', 'gy'), may hold values 0 or 1
- phase_rates: float32 [2], replicated, may hold values from 0.04 to 0.16
Outputs:
- level_gradient: float32 [128, 64, 128], P('gx', 'gy')
- velocity_gradient: float32 [3, 128, 64, 128], P(None, 'gx', 'gy')
The draws below stay inside these ranges and needn't reach their ends.
All inputs are finite; a program needn't handle non-finite values. No bound on the sum of `region_labels` on one device may be relied on, other than what follows from the above.
Results may differ from the reference program's by a relative error of at most 0.0001.
Values sent between devices are 32-bit elements; how exact they have to be, the bound alone decides.
No kernel may reach another device: no remote copies, remote signals or barrier semaphores. Data moves between devices by JAX's collectives and lax.ppermute only.
A program may use at most 128 MiB of HBM per device.

```python
import math
import jax
import jax.numpy as jnp

CX = 16
CY = 16
CZ = 128
STEPS = 2
TILES_X = 8
TILES_Y = 4
NX = 128
NY = 64


def set_ends(array, rng, low, high):
    place = [jax.random.randint(jax.random.fold_in(rng, axis), (), 0, length) for axis, length in enumerate(array.shape)]
    main_axis = array.shape.index(max(array.shape))
    beside = place[:main_axis] + [(place[main_axis] + 1) % array.shape[main_axis]] + place[main_axis + 1:]
    return array.at[tuple(place)].set(low).at[tuple(beside)].set(high)


def block_levels(own_key, shape, pieces, smallest, high):
    gain, own = 1.0, jax.random.fold_in(own_key, 6)
    for axis_at, blocks in pieces:
        steps = jnp.exp(jax.random.uniform(jax.random.fold_in(own, axis_at), (blocks,), jnp.float32, smallest / len(pieces), high / len(pieces)))
        gain = gain * jnp.repeat(steps, shape[axis_at] // blocks).reshape([-1 if axis == axis_at else 1 for axis in range(len(shape))])
    return gain


def scatter_about(rng, shape, deviation, most, pieces=(), kind=jnp.bfloat16):
    entries = deviation * jax.random.normal(rng, shape, jnp.float32)
    if pieces:
        entries = entries * block_levels(rng, shape, pieces, -0.22, 0.18)
    return jnp.clip(entries, -most, most).astype(kind)


def setup_inputs(seed: int = 0) -> dict:
    key_list = jax.random.split(jax.random.key(seed), 8)
    return {
        "level_cotangent": scatter_about(key_list[0], (NX, NY, CZ), 1.0, 6.0, ((0, 8), (1, 4)), jnp.float32),
        "velocity_cotangent": scatter_about(key_list[1], (3, NX, NY, CZ), 1.0, 6.0, ((1, 8), (2, 4)), jnp.float32),
        "fraction": jnp.clip(1.0 * jax.random.uniform(key_list[2], (STEPS, 3, NX, NY, CZ), jnp.float32) ** block_levels(key_list[2], (STEPS, 3, NX, NY, CZ), ((2, 8), (3, 4)), -0.2, 0.2), 0.0, 1.0),
        "shift_x": set_ends(jax.random.randint(key_list[3], (TILES_X, TILES_Y, STEPS), -2, 3), jax.random.fold_in(key_list[3], 1), -2, 2).astype(jnp.int32),
        "shift_y": set_ends(jax.random.randint(key_list[4], (TILES_X, TILES_Y, STEPS), -1, 2), jax.random.fold_in(key_list[4], 1), -1, 1).astype(jnp.int32),
        "region_labels": set_ends((jax.random.randint(key_list[5], (NX, NY, CZ), 0, 2) < 1).astype(jnp.int32), jax.random.fold_in(key_list[5], 1), 0, 1),
        "phase_rates": jnp.clip(jnp.exp(jax.random.uniform(key_list[6], (2,), jnp.float32, math.log(0.04), math.log(0.16))), 0.04, 0.16),
    }


BUOYANCY = 0.8


def cubic_weights(position):
    squared = position * position
    cubed = squared * position
    return ((2.0 * squared - cubed - position) * 0.5,
            (3.0 * cubed - 5.0 * squared + 2.0) * 0.5,
            (4.0 * squared - 3.0 * cubed + position) * 0.5,
            (cubed - squared) * 0.5)


def diffuse(values, cell_rate):
    summed = values
    for axis_index in (-3, -2, -1):
        for distance in (1, -1):
            neighbour = jnp.roll(values, distance, axis_index)
            neighbour_rate = jnp.roll(cell_rate, distance, axis_index)
            summed = summed + 0.5 * (cell_rate + neighbour_rate) * (neighbour - values)
    return summed


def to_tiles(values):
    lead_shape = values.shape[:-3]
    shaped = values.reshape(lead_shape + (TILES_X, CX, TILES_Y, CY, CZ))
    lead_count = len(lead_shape)
    axis_order = (lead_count, lead_count + 2) + tuple(range(lead_count)) + (lead_count + 1, lead_count + 3, lead_count + 4)
    return jnp.transpose(shaped, axis_order)


def spread_back(stacked, fractions, move_x, move_y):
    tiled = to_tiles(stacked)
    weights_x = cubic_weights(to_tiles(fractions[0]))
    weights_y = cubic_weights(to_tiles(fractions[1]))
    weights_z = cubic_weights(to_tiles(fractions[2]))
    patches = jnp.zeros((TILES_X, TILES_Y, 4, CX + 3, CY + 3, CZ), jnp.float32)
    for off_x in range(4):
        for off_y in range(4):
            weighted = tiled * (weights_x[off_x] * weights_y[off_y])[:, :, None]
            column = jnp.zeros_like(weighted)
            for off_z in range(4):
                column = column + jnp.roll(weighted * weights_z[off_z][:, :, None], off_z - 1, -1)
            patches = patches + jnp.pad(column, ((0, 0), (0, 0), (0, 0), (off_x, 3 - off_x), (off_y, 3 - off_y), (0, 0)))
    tile_x = jnp.arange(TILES_X, dtype=jnp.int32)[:, None]
    tile_y = jnp.arange(TILES_Y, dtype=jnp.int32)[None, :]
    target = ((tile_x + move_x.astype(jnp.int32)) % TILES_X) * TILES_Y + (tile_y + move_y.astype(jnp.int32)) % TILES_Y
    flat = patches.reshape((TILES_X * TILES_Y,) + patches.shape[2:])
    received = jax.ops.segment_sum(flat, target.reshape(-1).astype(jnp.int32), num_segments=TILES_X * TILES_Y).reshape(patches.shape)
    inner = received[:, :, :, 1:CX + 1]
    inner = inner.at[:, :, :, CX - 1:CX].add(jnp.roll(received[:, :, :, 0:1], -1, 0))
    inner = inner.at[:, :, :, 0:2].add(jnp.roll(received[:, :, :, CX + 1:CX + 3], 1, 0))
    folded = inner[:, :, :, :, 1:CY + 1]
    folded = folded.at[:, :, :, :, CY - 1:CY].add(jnp.roll(inner[:, :, :, :, 0:1], -1, 1))
    folded = folded.at[:, :, :, :, 0:2].add(jnp.roll(inner[:, :, :, :, CY + 1:CY + 3], 1, 1))
    return jnp.transpose(folded, (2, 0, 3, 1, 4, 5)).reshape(stacked.shape)


def reference(level_cotangent, velocity_cotangent, fraction, shift_x, shift_y, region_labels, phase_rates):
    cell_rate = jnp.where(region_labels == 1, phase_rates[1], phase_rates[0])
    level_now = level_cotangent
    velocity_now = velocity_cotangent
    for step_index in range(STEPS - 1, -1, -1):
        diffused = diffuse(diffuse(velocity_now, cell_rate), cell_rate)
        level_part = level_now + BUOYANCY * diffused[2]
        stacked = jnp.concatenate([level_part[None], diffused], 0)
        moved = spread_back(stacked, fraction[step_index], shift_x[:, :, step_index], shift_y[:, :, step_index])
        level_now = moved[0]
        velocity_now = moved[1:]
    return level_now, velocity_now
```

```python
import functools

import jax
import jax.numpy as jnp
from jax import lax
from jax.experimental import pallas as pl
from jax.experimental.pallas import tpu as pltpu
from jax.sharding import PartitionSpec as P

STEPS = 2
BUOYANCY = 0.8
FIELDS = 4
SUB = 8
VMEM = pl.BlockSpec(memory_space=pltpu.VMEM)
SMEM = pl.BlockSpec(memory_space=pltpu.SMEM)


def call(body, outs, args, specs, scratch=(), flops=1000000, name=None):
    moved = sum(a.size for a in args) * 4 + sum(o.size for o in outs) * 4
    return pl.pallas_call(
        body,
        out_shape=tuple(outs),
        in_specs=list(specs),
        out_specs=tuple(VMEM for _ in outs),
        scratch_shapes=list(scratch),
        compiler_params=pltpu.CompilerParams(vmem_limit_bytes=40 * 1024 * 1024),
        cost_estimate=pl.CostEstimate(flops=flops, bytes_accessed=moved, transcendentals=0),
        name=name,
    )(*args)


def f32(*shape):
    return jax.ShapeDtypeStruct(shape, jnp.float32)


def sublane(shape):
    return lax.broadcasted_iota(jnp.int32, shape, 0)


def turn(v, steps, axis):
    return pltpu.roll(v, steps % v.shape[axis], axis)


def cubic_weights(position):
    squared = position * position
    cubed = squared * position
    return (
        (2.0 * squared - cubed - position) * 0.5,
        (3.0 * cubed - 5.0 * squared + 2.0) * 0.5,
        (4.0 * squared - 3.0 * cubed + position) * 0.5,
        (cubed - squared) * 0.5,
    )


def prep_body(cx, cy, level, vel, labels, rates, state, rate, top, bot, left, right, c00, c01, c10, c11):
    pairs = cy // 2

    def row(x, _):
        state[x, pl.ds(0, cy, stride=FIELDS), :] = level[x]
        for f in range(3):
            state[x, pl.ds(f + 1, cy, stride=FIELDS), :] = vel[f, x]
        cell = jnp.where(labels[x] == 1, rates[1], rates[0])
        for f in range(FIELDS):
            rate[x, pl.ds(f, cy, stride=FIELDS), :] = cell
        return 0

    lax.fori_loop(0, cx, row, 0)

    def mixed(x, q):
        at = pl.ds(SUB * q, SUB)
        is_level = sublane(state[x, at, :].shape) % FIELDS == 0
        return jnp.where(is_level, rate[x, at, :], state[x, at, :])

    for k in range(2):
        for q in range(pairs):
            top[k * pairs + q] = mixed(k, q)
            bot[k * pairs + q] = mixed(cx - 2 + k, q)
    for x in range(cx):
        left[x] = mixed(x, 0)
        right[x] = mixed(x, pairs - 1)
    c00[0] = left[0]
    c01[0] = right[0]
    c10[0] = left[cx - 1]
    c11[0] = right[cx - 1]


def weights_body(cx, cy, step, fraction, out):
    def row(x, _):
        for d in range(3):
            for k, w in enumerate(cubic_weights(fraction[step, d, x])):
                for f in range(FIELDS):
                    out[4 * d + k, x, pl.ds(f, cy, stride=FIELDS), :] = w
        return 0

    lax.fori_loop(0, cx, row, 0)


def fill(pad, cx, pairs, own, xm, xp, ym, yp, c00, c01, c10, c11, change):
    wide = pairs + 2

    def row(x, _):
        for q in range(pairs):
            pad[(x + 2) * wide + q + 1] = own(x, q)
        pad[(x + 2) * wide] = change(ym[x])
        pad[(x + 2) * wide + pairs + 1] = change(yp[x])
        return 0

    lax.fori_loop(0, cx, row, 0)
    for k in range(2):
        for q in range(pairs):
            pad[k * wide + q + 1] = change(xm[k * pairs + q])
            pad[(cx + 2 + k) * wide + q + 1] = change(xp[k * pairs + q])
    pad[wide] = change(c00[0])
    pad[wide + pairs + 1] = change(c01[0])
    pad[(cx + 2) * wide] = change(c10[0])
    pad[(cx + 2) * wide + pairs + 1] = change(c11[0])


def coef_body(cx, pairs, rate, xm, xp, ym, yp, c00, c01, c10, c11, ax, yu, yd, zu, zd, c0, pad):
    wide = pairs + 2
    shape = pad.shape[1:]
    field = sublane(shape) % FIELDS
    half = sublane(shape) < FIELDS
    scale = jnp.where(field == 0, 0.0, 0.5)

    def spread_rate(v):
        v = jnp.where(field == 0, v, 0.0)
        v = v + turn(v, 1, 0)
        return v + turn(v, 2, 0)

    for k in (0, cx + 3):
        pad[k * wide] = jnp.zeros(shape, jnp.float32)
        pad[k * wide + pairs + 1] = jnp.zeros(shape, jnp.float32)
    fill(pad, cx, pairs, lambda x, q: rate[x * pairs + q], xm, xp, ym, yp, c00, c01, c10, c11, spread_rate)

    def faces(x, _):
        for j in range(wide):
            ax[x * wide + j] = (pad[x * wide + j] + pad[(x + 1) * wide + j]) * scale
        return 0

    lax.fori_loop(0, cx + 3, faces, 0)

    def row(x, _):
        flipped = [turn(pad[(x + 1) * wide + j], FIELDS, 0) for j in range(wide)]
        for j in range(wide):
            own = pad[(x + 1) * wide + j]
            up = jnp.where(half, flipped[j], flipped[min(j + 1, wide - 1)])
            down = jnp.where(half, flipped[max(j - 1, 0)], flipped[j])
            at = x * wide + j
            cyu = (own + up) * scale
            cyd = (own + down) * scale
            czu = (own + turn(own, -1, 1)) * scale
            czd = (own + turn(own, 1, 1)) * scale
            yu[at] = cyu
            yd[at] = cyd
            zu[at] = czu
            zd[at] = czd
            c0[at] = 1.0 - (ax[at] + ax[at + wide] + cyu + cyd + czu + czd)
        return 0

    lax.fori_loop(0, cx + 2, row, 0)


def sweep_row(src, base, lo, hi, coefs, at, half):
    ax, yu, yd, zu, zd, c0, wide = coefs
    own = {j: src[base + j] for j in range(max(lo - 1, 0), min(hi + 1, wide))}
    flipped = {j: turn(v, FIELDS, 0) for j, v in own.items()}
    for j in range(lo, hi):
        up = jnp.where(half, flipped[j], flipped.get(j + 1, flipped[j]))
        down = jnp.where(half, flipped.get(j - 1, flipped[j]), flipped[j])
        v = own[j]
        k = at + j
        total = c0[k] * v + ax[k] * src[base - wide + j] + ax[k + wide] * src[base + wide + j]
        total = total + yu[k] * up + yd[k] * down
        total = total + zu[k] * turn(v, -1, 1) + zd[k] * turn(v, 1, 1)
        yield j, total


def diffuse(cx, pairs, own, halos, coefs, pad, mid, g):
    wide = pairs + 2
    shape = pad.shape[1:]
    half = sublane(shape) < FIELDS
    lift = jnp.where(sublane(shape) % FIELDS == 0, BUOYANCY, 0.0)
    fill(pad, cx, pairs, lambda x, q: own[x * pairs + q], *halos, lambda v: v)
    coefs = coefs + (wide,)
    for r in (0, cx + 1):
        for j, v in sweep_row(pad, (r + 1) * wide, 1, pairs + 1, coefs, r * wide, half):
            mid[r * wide + j] = v

    def first(r, _):
        for j, v in sweep_row(pad, (r + 1) * wide, 0, wide, coefs, r * wide, half):
            mid[r * wide + j] = v
        return 0

    lax.fori_loop(1, cx + 1, first, 0)
    zero = jnp.zeros(shape, jnp.float32)
    for k in range(3 * pairs):
        g[k] = zero
        g[(cx + 3) * pairs + k] = zero

    def second(r, _):
        for j, v in sweep_row(mid, r * wide, 1, pairs + 1, coefs, r * wide, half):
            g[(r + 2) * pairs + j - 1] = v + lift * turn(v, -3, 0)
        return 0

    lax.fori_loop(1, cx + 1, second, 0)


def patch_row(g, w, cx, pairs, at):
    shape = g.shape[1:]
    half = sublane(shape) < FIELDS
    rows = [(at + 1 - a + 3, jnp.clip(at + 1 - a, 0, cx - 1)) for a in range(4)]
    before = None
    out = []
    zero = jnp.zeros(shape, jnp.float32)

    def finish(acc0, acc1, acc1_before):
        flipped = turn(acc1, FIELDS, 0) if acc1 is not None else zero
        flipped_before = turn(acc1_before, FIELDS, 0) if acc1_before is not None else zero
        value = jnp.where(half, flipped_before, flipped)
        return value if acc0 is None else acc0 + value

    p1 = p2 = p3 = p3_old = acc1_old = None
    for q in range(pairs):
        sums = [[None] * 4 for _ in range(4)]
        for a in range(4):
            padded, row = rows[a]
            k = pl.ds(SUB * q, SUB)
            h = g[padded * pairs + q] * w[a, row, k, :]
            wy = [w[4 + b, row, k, :] for b in range(4)]
            for c in range(4):
                hc = h * w[8 + c, row, k, :]
                for b in range(4):
                    t = hc * wy[b]
                    sums[b][c] = t if sums[b][c] is None else sums[b][c] + t
        p = []
        for b in range(4):
            s = sums[b]
            p.append((turn(s[0], -1, 1) + s[1]) + (turn(s[2], 1, 1) + turn(s[3], 2, 1)))
        acc1 = p[0] if p2 is None else p2 + p[0]
        acc0 = p1 if p3_old is None else p1 + p3_old
        out.append(finish(acc0, acc1, acc1_old))
        p3_old = p3
        p1, p2, p3 = p[1], p[2], p[3]
        acc1_old = acc1
    out.append(finish(p1 if p3_old is None else p1 + p3_old, p2, acc1_old))
    out.append(finish(p3, None, p2))
    return out


def spread(cx, pairs, rows_of, count, g, w, shift_x, shift_y, step, own, right, left, far):
    shape = g.shape[1:]
    move_x = shift_x[0, 0, step]
    move_y = shift_y[0, 0, step]
    here = jnp.where(move_y == 0, 1.0, 0.0)
    up = jnp.where(move_y == 1, 1.0, 0.0)
    down = jnp.where(move_y == -1, 1.0, 0.0)

    def row(i, _):
        out = patch_row(g, w, cx, pairs, rows_of(i))
        low, high = out[0], out[pairs + 1]
        for q in range(pairs):
            v = out[q + 1]
            o, r, l = v * here, v * up, v * down
            if q == 0:
                o = o + high * down
                r = r + high * here
            if q == pairs - 1:
                o = o + low * up
                l = l + low * here
            own[i * pairs + q] = o
            right[i * pairs + q] = r
            left[i * pairs + q] = l
        far[i] = high * up + low * down
        return 0

    lax.fori_loop(0, count, row, 0)
    mx = jnp.full(shape, move_x.astype(jnp.float32))
    right[count * pairs] = mx
    left[count * pairs] = mx
    far[count] = mx
    far[count + 1] = jnp.full(shape, move_y.astype(jnp.float32))


def diffuse_spread_body(cx, pairs, step, rows_of, count, *refs):
    own, halos, coefs, w, sx, sy = refs[0], refs[1:9], refs[9:15], refs[15], refs[16], refs[17]
    o, r, l, far, g, pad, mid = refs[18:]
    diffuse(cx, pairs, own, halos, coefs, pad, mid, g)
    spread(cx, pairs, rows_of, count, g, w, sx, sy, step, o, r, l, far)


def spread_body(cx, pairs, step, rows_of, count, g, w, sx, sy, o, r, l, far):
    spread(cx, pairs, rows_of, count, g, w, sx, sy, step, o, r, l, far)


def gather_body(pairs, step, main, rim_at, edge_of, has_high, has_low, *refs):
    own, right, left, far_low, far_high, sx, parity = refs[:7]
    e1, e0, f, k, t0, x3 = refs[7:]
    shape = own.shape[1:]
    count = own.shape[0] // pairs
    mine = jnp.full(shape, sx[0, 0, step].astype(jnp.float32))
    moves = (mine, right[count * pairs], left[count * pairs])
    far_moves = (far_low[count], far_high[count])
    far_gates = (far_low[count + 1] == 1.0, far_high[count + 1] == -1.0)
    side = parity[0]
    targets = (side, -side, 2 * side, -2 * side, 0)
    outs = (e1, e0, f, k, t0)

    def hit(move, t):
        t = t.astype(jnp.float32) if hasattr(t, "astype") else float(t)
        return jnp.where(move == t, 1.0, 0.0)

    def total(masks, fars, i, q):
        v = masks[0] * own[i * pairs + q] + masks[1] * right[i * pairs + q] + masks[2] * left[i * pairs + q]
        if q == 0:
            v = v + fars[0] * far_low[i]
        if q == pairs - 1:
            v = v + fars[1] * far_high[i]
        return v

    def masks_of(t):
        masks = [hit(m, t) for m in moves]
        fars = [jnp.where(gate, hit(m, t), 0.0) for gate, m in zip(far_gates, far_moves)]
        return masks, fars

    for out, t in zip(outs, targets):
        masks, fars = masks_of(t)

        def row(i, _, out=out, masks=masks, fars=fars):
            for q in range(pairs):
                out[i * pairs + q] = total(masks, fars, i + rim_at, q)
            return 0

        lax.fori_loop(0, main, row, 0)
        masks, fars = masks_of(t + edge_of)
        for source, row_at in (has_high or ()) + (has_low or ()):
            for q in range(pairs):
                out[row_at * pairs + q] = out[row_at * pairs + q] + total(masks, fars, source, q)
    masks, fars = masks_of(2 if has_high else -2)
    for n, (source, _) in enumerate((has_high or ()) + (has_low or ())):
        for q in range(pairs):
            x3[n * pairs + q] = total(masks, fars, source, q)


def merge(cx, pairs, main, parts, state):
    (t0a, e0a, fa, da, xa), (t0b, e0b, fb, db, xb) = parts
    for base, (t0, e0, f, d) in ((0, (t0a, e0a, fa, da)), (main[0], (t0b, e0b, fb, db))):

        def row(i, _, base=base, t0=t0, e0=e0, f=f, d=d):
            for q in range(pairs):
                at = i * pairs + q
                state((base + i), q, (t0[at] + e0[at]) + (f[at] + d[at]), False)
            return 0

        lax.fori_loop(0, main[0] if base == 0 else main[1], row, 0)
    for q in range(pairs):
        for k in range(2):
            state(k, q, xa[k * pairs + q], True)
        state(cx - 1, q, xb[q], True)


def merge_body(cx, pairs, main, *refs):
    parts = (refs[0:5], refs[5:10])
    out, top, bot, left, right, c00, c01, c10, c11 = refs[10:]

    def put(x, q, v, add):
        at = x * pairs + q
        out[at] = out[at] + v if add else v

    merge(cx, pairs, main, parts, put)
    for k in range(2 * pairs):
        top[k] = out[k]
        bot[k] = out[(cx - 2) * pairs + k]
    for x in range(cx):
        left[x] = out[x * pairs]
        right[x] = out[x * pairs + pairs - 1]
    c00[0] = left[0]
    c01[0] = right[0]
    c10[0] = left[cx - 1]
    c11[0] = right[cx - 1]


def finish_body(cx, cy, pairs, main, *refs):
    parts = (refs[0:5], refs[5:10])
    level, vel, out = refs[10:]

    def put(x, q, v, add):
        at = pl.ds(SUB * q, SUB)
        out[x, at, :] = out[x, at, :] + v if add else v

    merge(cx, pairs, main, parts, put)

    def row(x, _):
        level[x] = out[x, pl.ds(0, cy, stride=FIELDS), :]
        for f in range(3):
            vel[f, x] = out[x, pl.ds(f + 1, cy, stride=FIELDS), :]
        return 0

    lax.fori_loop(0, cx, row, 0)


def moved(value, axis, steps):
    count = lax.axis_size(axis)
    return lax.ppermute(value, axis, [(i, (i + steps) % count) for i in range(count)])


def moved_both(value, step_x, step_y):
    nx, ny = lax.axis_size("gx"), lax.axis_size("gy")
    pairs = [
        (x * ny + y, ((x + step_x) % nx) * ny + (y + step_y) % ny)
        for x in range(nx)
        for y in range(ny)
    ]
    return lax.ppermute(value, ("gx", "gy"), pairs)


def swapped(value):
    return lax.ppermute(value, "gx", [(i, i ^ 1) for i in range(lax.axis_size("gx"))])


def crossed(value, sign):
    count = lax.axis_size("gx")
    return lax.ppermute(
        value, "gx", [(i, (i + (2 if i % 2 else -2) * sign) % count) for i in range(count)]
    )


def exchange(top, bot, left, right, c00, c01, c10, c11):
    xm = moved(bot, "gx", 1)
    xp = moved(top, "gx", -1)
    ym = moved(right, "gy", 1)
    yp = moved(left, "gy", -1)
    mm = moved_both(c11, 1, 1)
    mp = moved_both(c10, 1, -1)
    pm = moved_both(c01, -1, 1)
    pp = moved_both(c00, -1, -1)
    return xm, xp, ym, yp, mm, mp, pm, pp


def on_device(level, vel, fraction, shift_x, shift_y, labels, rates):
    cx, cy, cz = level.shape
    pairs = cy // 2
    wide = pairs + 2
    ny = lax.axis_size("gy")
    parity = (2 * (lax.axis_index("gx") % 2) - 1).astype(jnp.int32).reshape(1)
    first = cx // 2
    main = (first, cx - first)

    def plane(n):
        return f32(n, SUB, cz)

    def scratch(n):
        return pltpu.VMEM((n, SUB, cz), jnp.float32)

    halo_outs = (
        [plane(2 * pairs)] * 2 + [plane(cx)] * 2 + [plane(1)] * 4
    )
    state, rate, *edges = call(
        functools.partial(prep_body, cx, cy),
        [f32(cx, FIELDS * cy, cz)] * 2 + halo_outs,
        (level, vel, labels, rates),
        [VMEM, VMEM, VMEM, SMEM],
        name="prep",
    )
    state = state.reshape(cx * pairs, SUB, cz)
    rate = rate.reshape(cx * pairs, SUB, cz)
    halos = exchange(*edges)
    weights = [
        call(
            functools.partial(weights_body, cx, cy, s),
            [f32(12, cx, FIELDS * cy, cz)],
            (fraction,),
            [VMEM],
            name="weights%d" % s,
        )[0]
        for s in range(STEPS)
    ]
    coefs = call(
        functools.partial(coef_body, cx, pairs),
        [plane((cx + 3) * wide)] + [plane((cx + 2) * wide)] * 5,
        (rate, *halos),
        [VMEM] * 9,
        [scratch((cx + 4) * wide)],
        name="coefs",
    )

    def rows_a(i):
        return jnp.where(i < 2, cx + i, i - 2)

    def rows_b(i):
        return jnp.where(i < 1, -1, first - 1 + i)

    counts = (main[0] + 2, main[1] + 1)
    for step in range(STEPS - 1, -1, -1):
        chunks = []
        spec_tail = [VMEM, SMEM, SMEM]

        def outs(n):
            return [plane(n * pairs), plane(n * pairs + 1), plane(n * pairs + 1), plane(n + 2)]

        *sent_a, g = call(
            functools.partial(diffuse_spread_body, cx, pairs, step, rows_a, counts[0]),
            outs(counts[0]) + [plane((cx + 6) * pairs)],
            (state, *halos, *coefs, weights[step], shift_x, shift_y),
            [VMEM] * 15 + spec_tail,
            [scratch((cx + 4) * wide), scratch((cx + 2) * wide)],
            flops=20000000,
            name="diffuse_spread_a%d" % step,
        )
        sent_b = call(
            functools.partial(spread_body, cx, pairs, step, rows_b, counts[1]),
            outs(counts[1]),
            (g, weights[step], shift_x, shift_y),
            [VMEM] + spec_tail,
            flops=10000000,
            name="spread_b%d" % step,
        )
        for n, (own, right, left, far) in enumerate((sent_a, sent_b)):
            right = moved(right, "gy", 1)
            left = moved(left, "gy", -1)
            far_low = moved(far, "gy", 2)
            far_high = far_low if ny == 4 else moved(far, "gy", -2)
            if n == 0:
                args = (2, -1, ((0, 0), (1, 1)), None)
            else:
                args = (1, 1, None, ((0, main[1] - 1),))
            e1, e0, f, k, t0, x3 = call(
                functools.partial(gather_body, pairs, step, main[n], *args),
                [plane(main[n] * pairs)] * 5 + [plane((2 if n == 0 else 1) * pairs)],
                (own, right, left, far_low, far_high, shift_x, parity),
                [VMEM] * 5 + [SMEM] * 2,
                flops=3000000,
                name="gather%d_%d" % (n, step),
            )
            e1 = swapped(e1)
            f = crossed(f, 1)
            x3 = moved(x3, "gx", 3 if n == 0 else -3)
            e0 = swapped(e0)
            d = crossed(k + e1, -1)
            chunks += [t0, e0, f, d, x3]
        if step:
            state, *edges = call(
                functools.partial(merge_body, cx, pairs, main),
                [plane(cx * pairs)] + halo_outs,
                chunks,
                [VMEM] * 10,
                name="merge%d" % step,
            )
            halos = exchange(*edges)
        else:
            return call(
                functools.partial(finish_body, cx, cy, pairs, main),
                [f32(cx, cy, cz), f32(3, cx, cy, cz)],
                chunks,
                [VMEM] * 10,
                [pltpu.VMEM((cx, FIELDS * cy, cz), jnp.float32)],
                name="finish",
            )


def solution(mesh):
    in_specs = (
        P("gx", "gy", None),
        P(None, "gx", "gy", None),
        P(None, None, "gx", "gy", None),
        P("gx", "gy", None),
        P("gx", "gy", None),
        P("gx", "gy", None),
        P(),
    )
    out_specs = (P("gx", "gy", None), P(None, "gx", "gy", None))
    return jax.shard_map(
        on_device, mesh=mesh, in_specs=in_specs, out_specs=out_specs, check_vma=False
    )
```

```python
import functools

import jax
import jax.numpy as jnp
from jax import lax
from jax.experimental import pallas as pl
from jax.experimental.pallas import tpu as pltpu
from jax.sharding import PartitionSpec as P


STEPS = 2
BUOYANCY = 0.8
FIELDS = 4
SUB = 8
VMEM = pl.BlockSpec(memory_space=pltpu.VMEM)
SMEM = pl.BlockSpec(memory_space=pltpu.SMEM)


def call(body, outs, args, specs, scratch=(), flops=1000000):
    moved = sum(a.size for a in args) * 4 + sum(o.size for o in outs) * 4
    return pl.pallas_call(
        body,
        out_shape=tuple(outs),
        in_specs=list(specs),
        out_specs=tuple(VMEM for _ in outs),
        scratch_shapes=list(scratch),
        compiler_params=pltpu.CompilerParams(vmem_limit_bytes=8 * 1024 * 1024),
        cost_estimate=pl.CostEstimate(flops=flops, bytes_accessed=moved, transcendentals=0),
    )(*args)


def f32(*shape):
    return jax.ShapeDtypeStruct(shape, jnp.float32)


def sublane(shape):
    return lax.broadcasted_iota(jnp.int32, shape, 0)


def turn(v, steps, axis):
    return pltpu.roll(v, steps % v.shape[axis], axis)


def cubic_weights(position):
    squared = position * position
    cubed = squared * position
    return (
        (2.0 * squared - cubed - position) * 0.5,
        (3.0 * cubed - 5.0 * squared + 2.0) * 0.5,
        (4.0 * squared - 3.0 * cubed + position) * 0.5,
        (cubed - squared) * 0.5,
    )


def prep_body(cx, cy, *refs):
    hbm, (state, rate, left, right), local, sem = refs[:4], refs[4:8], refs[8:12], refs[12]
    pairs = cy // 2
    copies = [pltpu.make_async_copy(a, b, sem.at[n]) for n, (a, b) in enumerate(zip(hbm, local))]
    for copy in copies:
        copy.start()
    for copy in copies:
        copy.wait()
    level, vel, labels, rates = local

    def row(x, _):
        state[x, pl.ds(0, cy, stride=FIELDS), :] = level[x]
        for f in range(3):
            state[x, pl.ds(f + 1, cy, stride=FIELDS), :] = vel[f, x]
        cell = jnp.where(labels[x] == 1, rates[1], rates[0])
        for f in range(FIELDS):
            rate[x, pl.ds(f, cy, stride=FIELDS), :] = cell
        return 0

    lax.fori_loop(0, cx, row, 0)

    def mixed(x, q):
        at = pl.ds(SUB * q, SUB)
        is_level = sublane(state[x, at, :].shape) % FIELDS == 0
        return jnp.where(is_level, rate[x, at, :], state[x, at, :])

    for x in range(cx):
        left[x] = mixed(x, 0)
        right[x] = mixed(x, pairs - 1)


def edge_rows_body(cx, pairs, mix, *refs):
    sources, (top, bot) = refs[:-2], refs[-2:]
    state, ym, yp = sources[0], sources[-2], sources[-1]
    wide = pairs + 2
    for out, rows in ((top, (0, 1)), (bot, (cx - 2, cx - 1))):
        for k, x in enumerate(rows):
            out[k * wide] = ym[x]
            out[k * wide + pairs + 1] = yp[x]
            for q in range(pairs):
                v = state[x * pairs + q]
                if mix:
                    v = jnp.where(sublane(v.shape) % FIELDS == 0, sources[1][x * pairs + q], v)
                out[k * wide + q + 1] = v


def weights_body(cx, cy, step, fraction, out):
    def row(x, _):
        for d in range(3):
            for k, w in enumerate(cubic_weights(fraction[step, d, x])):
                for f in range(FIELDS):
                    out[4 * d + k, x, pl.ds(f, cy, stride=FIELDS), :] = w
        return 0

    lax.fori_loop(0, cx, row, 0)


def fill(pad, cx, pairs, own, xm, xp, ym, yp, change):
    wide = pairs + 2

    def row(x, _):
        for q in range(pairs):
            pad[(x + 2) * wide + q + 1] = own(x, q)
        pad[(x + 2) * wide] = change(ym[x])
        pad[(x + 2) * wide + pairs + 1] = change(yp[x])
        return 0

    lax.fori_loop(0, cx, row, 0)
    for k in range(2 * wide):
        pad[k] = change(xm[k])
        pad[(cx + 2) * wide + k] = change(xp[k])


def coef_body(cx, pairs, rate, xm, xp, ym, yp, ax, yu, yd, zu, zd, c0, pad):
    wide = pairs + 2
    shape = pad.shape[1:]
    field = sublane(shape) % FIELDS
    half = sublane(shape) < FIELDS
    scale = jnp.where(field == 0, 0.0, 0.5)

    def spread_rate(v):
        v = jnp.where(field == 0, v, 0.0)
        v = v + turn(v, 1, 0)
        return v + turn(v, 2, 0)

    fill(pad, cx, pairs, lambda x, q: rate[x * pairs + q], xm, xp, ym, yp, spread_rate)

    def faces(x, _):
        for j in range(wide):
            ax[x * wide + j] = (pad[x * wide + j] + pad[(x + 1) * wide + j]) * scale
        return 0

    lax.fori_loop(0, cx + 3, faces, 0)

    def row(x, _):
        flipped = [turn(pad[(x + 1) * wide + j], FIELDS, 0) for j in range(wide)]
        for j in range(wide):
            own = pad[(x + 1) * wide + j]
            up = jnp.where(half, flipped[j], flipped[min(j + 1, wide - 1)])
            down = jnp.where(half, flipped[max(j - 1, 0)], flipped[j])
            at = x * wide + j
            cyu = (own + up) * scale
            cyd = (own + down) * scale
            czu = (own + turn(own, -1, 1)) * scale
            czd = (own + turn(own, 1, 1)) * scale
            yu[at] = cyu
            yd[at] = cyd
            zu[at] = czu
            zd[at] = czd
            c0[at] = 1.0 - (ax[at] + ax[at + wide] + cyu + cyd + czu + czd)
        return 0

    lax.fori_loop(0, cx + 2, row, 0)


def sweep_row(src, base, lo, hi, coefs, at, half):
    ax, yu, yd, zu, zd, c0, wide = coefs
    own = {j: src[base + j] for j in range(max(lo - 1, 0), min(hi + 1, wide))}
    flipped = {j: turn(v, FIELDS, 0) for j, v in own.items()}
    for j in range(lo, hi):
        up = jnp.where(half, flipped[j], flipped.get(j + 1, flipped[j]))
        down = jnp.where(half, flipped.get(j - 1, flipped[j]), flipped[j])
        v = own[j]
        k = at + j
        total = c0[k] * v + ax[k] * src[base - wide + j] + ax[k + wide] * src[base + wide + j]
        total = total + yu[k] * up + yd[k] * down
        total = total + zu[k] * turn(v, -1, 1) + zd[k] * turn(v, 1, 1)
        yield j, total


def diffuse(cx, pairs, own, halos, coefs, pad, mid, g):
    wide = pairs + 2
    shape = pad.shape[1:]
    half = sublane(shape) < FIELDS
    lift = jnp.where(sublane(shape) % FIELDS == 0, BUOYANCY, 0.0)
    fill(pad, cx, pairs, lambda x, q: own[x * pairs + q], *halos, lambda v: v)
    coefs = coefs + (wide,)
    for r in (0, cx + 1):
        for j, v in sweep_row(pad, (r + 1) * wide, 1, pairs + 1, coefs, r * wide, half):
            mid[r * wide + j] = v

    def first(r, _):
        for j, v in sweep_row(pad, (r + 1) * wide, 0, wide, coefs, r * wide, half):
            mid[r * wide + j] = v
        return 0

    lax.fori_loop(1, cx + 1, first, 0)
    zero = jnp.zeros(shape, jnp.float32)
    for k in range(3 * pairs):
        g[k] = zero
        g[(cx + 3) * pairs + k] = zero

    def second(r, _):
        for j, v in sweep_row(mid, r * wide, 1, pairs + 1, coefs, r * wide, half):
            g[(r + 2) * pairs + j - 1] = v + lift * turn(v, -3, 0)
        return 0

    lax.fori_loop(1, cx + 1, second, 0)


def patch_row(g, w, cx, pairs, at):
    shape = g.shape[1:]
    half = sublane(shape) < FIELDS
    rows = [(at + 1 - a + 3, jnp.clip(at + 1 - a, 0, cx - 1)) for a in range(4)]
    out = []
    zero = jnp.zeros(shape, jnp.float32)

    def finish(acc0, acc1, acc1_before):
        flipped = turn(acc1, FIELDS, 0) if acc1 is not None else zero
        flipped_before = turn(acc1_before, FIELDS, 0) if acc1_before is not None else zero
        value = jnp.where(half, flipped_before, flipped)
        return value if acc0 is None else acc0 + value

    p1 = p2 = p3 = p3_old = acc1_old = None
    for q in range(pairs):
        sums = [[None] * 4 for _ in range(4)]
        for a in range(4):
            padded, row = rows[a]
            k = pl.ds(SUB * q, SUB)
            h = g[padded * pairs + q] * w[a, row, k, :]
            wy = [w[4 + b, row, k, :] for b in range(4)]
            for c in range(4):
                hc = h * w[8 + c, row, k, :]
                for b in range(4):
                    t = hc * wy[b]
                    sums[b][c] = t if sums[b][c] is None else sums[b][c] + t
        p = []
        for b in range(4):
            s = sums[b]
            p.append((turn(s[0], -1, 1) + s[1]) + (turn(s[2], 1, 1) + turn(s[3], 2, 1)))
        acc1 = p[0] if p2 is None else p2 + p[0]
        acc0 = p1 if p3_old is None else p1 + p3_old
        out.append(finish(acc0, acc1, acc1_old))
        p3_old = p3
        p1, p2, p3 = p[1], p[2], p[3]
        acc1_old = acc1
    out.append(finish(p1 if p3_old is None else p1 + p3_old, p2, acc1_old))
    out.append(finish(p3, None, p2))
    return out


def spread(cx, pairs, rows_of, count, g, w, shift_x, shift_y, step, own, right, left, far):
    shape = g.shape[1:]
    move_x = shift_x[0, 0, step]
    move_y = shift_y[0, 0, step]
    here = jnp.where(move_y == 0, 1.0, 0.0)
    up = jnp.where(move_y == 1, 1.0, 0.0)
    down = jnp.where(move_y == -1, 1.0, 0.0)

    def row(i, _):
        out = patch_row(g, w, cx, pairs, rows_of(i))
        low, high = out[0], out[pairs + 1]
        for q in range(pairs):
            v = out[q + 1]
            o, r, l = v * here, v * up, v * down
            if q == 0:
                o = o + high * down
                r = r + high * here
            if q == pairs - 1:
                o = o + low * up
                l = l + low * here
            own[i * pairs + q] = o
            right[i * pairs + q] = r
            left[i * pairs + q] = l
        far[i] = high * up + low * down
        return 0

    lax.fori_loop(0, count, row, 0)
    mx = jnp.full(shape, move_x.astype(jnp.float32))
    right[count * pairs] = mx
    left[count * pairs] = mx
    far[count] = mx
    far[count + 1] = jnp.full(shape, move_y.astype(jnp.float32))


def diffuse_spread_body(cx, pairs, step, rows_of, count, *refs):
    own, halos, coefs, w, sx, sy = refs[0], refs[1:5], refs[5:11], refs[11], refs[12], refs[13]
    o, r, l, far, g, pad, mid = refs[14:]
    diffuse(cx, pairs, own, halos, coefs, pad, mid, g)
    spread(cx, pairs, rows_of, count, g, w, sx, sy, step, o, r, l, far)


def spread_body(cx, pairs, step, rows_of, count, g, w, sx, sy, o, r, l, far):
    spread(cx, pairs, rows_of, count, g, w, sx, sy, step, o, r, l, far)


def gather_body(pairs, step, main, rim_at, edge_of, has_high, has_low, *refs):
    own, right, left, far_low, far_high, sx = refs[:6]
    e1, e0, f, k, t0, x3 = refs[6:]
    shape = own.shape[1:]
    count = own.shape[0] // pairs
    mine = jnp.full(shape, sx[0, 0, step].astype(jnp.float32))
    moves = (mine, right[count * pairs], left[count * pairs])
    far_moves = (far_low[count], far_high[count])
    far_gates = (far_low[count + 1] == 1.0, far_high[count + 1] == -1.0)
    side = 2 * lax.rem(lax.axis_index("gx"), 2) - 1
    targets = (side, -side, 2 * side, -2 * side, 0)
    outs = (e1, e0, f, k, t0)

    def hit(move, t):
        t = t.astype(jnp.float32) if hasattr(t, "astype") else float(t)
        return jnp.where(move == t, 1.0, 0.0)

    def total(masks, fars, i, q):
        v = masks[0] * own[i * pairs + q] + masks[1] * right[i * pairs + q] + masks[2] * left[i * pairs + q]
        if q == 0:
            v = v + fars[0] * far_low[i]
        if q == pairs - 1:
            v = v + fars[1] * far_high[i]
        return v

    def masks_of(t):
        masks = [hit(m, t) for m in moves]
        fars = [jnp.where(gate, hit(m, t), 0.0) for gate, m in zip(far_gates, far_moves)]
        return masks, fars

    for out, t in zip(outs, targets):
        masks, fars = masks_of(t)

        def row(i, _, out=out, masks=masks, fars=fars):
            for q in range(pairs):
                out[i * pairs + q] = total(masks, fars, i + rim_at, q)
            return 0

        lax.fori_loop(0, main, row, 0)
        masks, fars = masks_of(t + edge_of)
        for source, row_at in (has_high or ()) + (has_low or ()):
            for q in range(pairs):
                out[row_at * pairs + q] = out[row_at * pairs + q] + total(masks, fars, source, q)
    masks, fars = masks_of(2 if has_high else -2)
    for n, (source, _) in enumerate((has_high or ()) + (has_low or ())):
        for q in range(pairs):
            x3[n * pairs + q] = total(masks, fars, source, q)


def add_body(a, b, out):
    def rows(i, _):
        for j in range(8):
            out[i * 8 + j] = a[i * 8 + j] + b[i * 8 + j]
        return 0

    lax.fori_loop(0, out.shape[0] // 8, rows, 0)


def merge(cx, pairs, main, parts, state):
    (t0a, e0a, fa, da, xa), (t0b, e0b, fb, db, xb) = parts
    for base, (t0, e0, f, d) in ((0, (t0a, e0a, fa, da)), (main[0], (t0b, e0b, fb, db))):

        def row(i, _, base=base, t0=t0, e0=e0, f=f, d=d):
            for q in range(pairs):
                at = i * pairs + q
                state((base + i), q, (t0[at] + e0[at]) + (f[at] + d[at]), False)
            return 0

        lax.fori_loop(0, main[0] if base == 0 else main[1], row, 0)
    for q in range(pairs):
        for k in range(2):
            state(k, q, xa[k * pairs + q], True)
        state(cx - 1, q, xb[q], True)


def merge_body(cx, pairs, main, *refs):
    parts = (refs[0:5], refs[5:10])
    out, left, right = refs[10:]

    def put(x, q, v, add):
        at = x * pairs + q
        out[at] = out[at] + v if add else v

    merge(cx, pairs, main, parts, put)
    for x in range(cx):
        left[x] = out[x * pairs]
        right[x] = out[x * pairs + pairs - 1]


def finish_body(cx, cy, pairs, main, *refs):
    parts = (refs[0:5], refs[5:10])
    level, vel, out = refs[10:]

    def put(x, q, v, add):
        at = pl.ds(SUB * q, SUB)
        out[x, at, :] = out[x, at, :] + v if add else v

    merge(cx, pairs, main, parts, put)

    def row(x, _):
        level[x] = out[x, pl.ds(0, cy, stride=FIELDS), :]
        for f in range(3):
            vel[f, x] = out[x, pl.ds(f + 1, cy, stride=FIELDS), :]
        return 0

    lax.fori_loop(0, cx, row, 0)


def moved(value, axis, steps):
    count = lax.axis_size(axis)
    return lax.ppermute(value, axis, [(i, (i + steps) % count) for i in range(count)])


def swapped(value):
    return lax.ppermute(value, "gx", [(i, i ^ 1) for i in range(lax.axis_size("gx"))])


def crossed(value, sign):
    count = lax.axis_size("gx")
    return lax.ppermute(
        value, "gx", [(i, (i + (2 if i % 2 else -2) * sign) % count) for i in range(count)]
    )


def exchange(cx, pairs, states, left, right):
    ym = moved(right, "gy", 1)
    yp = moved(left, "gy", -1)
    shape = f32(2 * (pairs + 2), *left.shape[1:])
    top, bot = call(
        functools.partial(edge_rows_body, cx, pairs, len(states) == 2),
        [shape] * 2,
        (*states, ym, yp),
        [VMEM] * (len(states) + 2),
    )
    xm = moved(bot, "gx", 1)
    xp = moved(top, "gx", -1)
    return xm, xp, ym, yp


def on_device(level, vel, fraction, shift_x, shift_y, labels, rates):
    cx, cy, cz = level.shape
    pairs = cy // 2
    wide = pairs + 2
    ny = lax.axis_size("gy")
    first = cx // 2
    main = (first, cx - first)

    def plane(n):
        return f32(n, SUB, cz)

    def scratch(n):
        return pltpu.VMEM((n, SUB, cz), jnp.float32)

    halo_outs = [plane(cx)] * 2
    local = [pltpu.VMEM(a.shape, a.dtype) for a in (level, vel, labels)]
    state, rate, *edges = call(
        functools.partial(prep_body, cx, cy),
        [f32(cx, FIELDS * cy, cz)] * 2 + halo_outs,
        (level, vel, labels, rates),
        [pl.BlockSpec(memory_space=pltpu.HBM)] * 4,
        local + [pltpu.SMEM(rates.shape, rates.dtype), pltpu.SemaphoreType.DMA((4,))],
    )
    state = state.reshape(cx * pairs, SUB, cz)
    rate = rate.reshape(cx * pairs, SUB, cz)
    halos = exchange(cx, pairs, (state, rate), *edges)
    weights = [
        call(
            functools.partial(weights_body, cx, cy, s),
            [f32(12, cx, FIELDS * cy, cz)],
            (fraction,),
            [VMEM],
        )[0]
        for s in range(STEPS)
    ]
    coefs = call(
        functools.partial(coef_body, cx, pairs),
        [plane((cx + 3) * wide)] + [plane((cx + 2) * wide)] * 5,
        (rate, *halos),
        [VMEM] * 5,
        [scratch((cx + 4) * wide)],
    )

    def rows_a(i):
        return jnp.where(i < 2, cx + i, i - 2)

    def rows_b(i):
        return jnp.where(i < 1, -1, first - 1 + i)

    counts = (main[0] + 2, main[1] + 1)
    for step in range(STEPS - 1, -1, -1):
        chunks = []
        spec_tail = [VMEM, SMEM, SMEM]

        def outs(n):
            return [plane(n * pairs), plane(n * pairs + 1), plane(n * pairs + 1), plane(n + 2)]

        *sent_a, g = call(
            functools.partial(diffuse_spread_body, cx, pairs, step, rows_a, counts[0]),
            outs(counts[0]) + [plane((cx + 6) * pairs)],
            (state, *halos, *coefs, weights[step], shift_x, shift_y),
            [VMEM] * 11 + spec_tail,
            [scratch((cx + 4) * wide), scratch((cx + 2) * wide)],
            flops=20000000,
        )
        sent_b = call(
            functools.partial(spread_body, cx, pairs, step, rows_b, counts[1]),
            outs(counts[1]),
            (g, weights[step], shift_x, shift_y),
            [VMEM] + spec_tail,
            flops=10000000,
        )
        for n, (own, right, left, far) in enumerate((sent_a, sent_b)):
            if n:
                own, _ = lax.optimization_barrier((own, chunks[0]))
            right = moved(right, "gy", 1)
            left = moved(left, "gy", -1)
            far_low = moved(far, "gy", 2)
            far_high = far_low if ny == 4 else moved(far, "gy", -2)
            if n == 0:
                args = (2, -1, ((0, 0), (1, 1)), None)
            else:
                args = (1, 1, None, ((0, main[1] - 1),))
            e1, e0, f, k, t0, x3 = call(
                functools.partial(gather_body, pairs, step, main[n], *args),
                [plane(main[n] * pairs)] * 5 + [plane((2 if n == 0 else 1) * pairs)],
                (own, right, left, far_low, far_high, shift_x),
                [VMEM] * 5 + [SMEM],
                flops=3000000,
            )
            e1 = swapped(e1)
            f = crossed(f, 1)
            e0 = swapped(e0)
            x3 = moved(x3, "gx", 3 if n == 0 else -3)
            (d,) = call(add_body, [plane(main[n] * pairs)], (k, e1), [VMEM] * 2)
            d = crossed(d, -1)
            chunks += [t0, e0, f, d, x3]
        if step:
            state, *edges = call(
                functools.partial(merge_body, cx, pairs, main),
                [plane(cx * pairs)] + halo_outs,
                chunks,
                [VMEM] * 10,
            )
            halos = exchange(cx, pairs, (state,), *edges)
        else:
            return call(
                functools.partial(finish_body, cx, cy, pairs, main),
                [f32(cx, cy, cz), f32(3, cx, cy, cz)],
                chunks,
                [VMEM] * 10,
                [pltpu.VMEM((cx, FIELDS * cy, cz), jnp.float32)],
            )


def solution(mesh):
    in_specs = (
        P("gx", "gy", None),
        P(None, "gx", "gy", None),
        P(None, None, "gx", "gy", None),
        P("gx", "gy", None),
        P("gx", "gy", None),
        P("gx", "gy", None),
        P(),
    )
    out_specs = (P("gx", "gy", None), P(None, "gx", "gy", None))
    return jax.shard_map(
        on_device, mesh=mesh, in_specs=in_specs, out_specs=out_specs, check_vma=False
    )
```

```python
import functools

import jax
import jax.numpy as jnp
from jax import lax
from jax.experimental import pallas as pl
from jax.experimental.pallas import tpu as pltpu
from jax.sharding import PartitionSpec as P


STEPS = 2
BUOYANCY = 0.8
FIELDS = 4
SUB = 8
VMEM = pl.BlockSpec(memory_space=pltpu.VMEM)
SMEM = pl.BlockSpec(memory_space=pltpu.SMEM)


def call(body, outs, args, specs, scratch=(), flops=1000000):
    moved = sum(a.size for a in args) * 4 + sum(o.size for o in outs) * 4
    return pl.pallas_call(
        body,
        out_shape=tuple(outs),
        in_specs=list(specs),
        out_specs=tuple(VMEM for _ in outs),
        scratch_shapes=list(scratch),
        compiler_params=pltpu.CompilerParams(vmem_limit_bytes=8 * 1024 * 1024),
        cost_estimate=pl.CostEstimate(flops=flops, bytes_accessed=moved, transcendentals=0),
    )(*args)


def f32(*shape):
    return jax.ShapeDtypeStruct(shape, jnp.float32)


def sublane(shape):
    return lax.broadcasted_iota(jnp.int32, shape, 0)


def turn(v, steps, axis):
    return pltpu.roll(v, steps % v.shape[axis], axis)


def cubic_weights(position):
    squared = position * position
    cubed = squared * position
    return (
        (2.0 * squared - cubed - position) * 0.5,
        (3.0 * cubed - 5.0 * squared + 2.0) * 0.5,
        (4.0 * squared - 3.0 * cubed + position) * 0.5,
        (cubed - squared) * 0.5,
    )


def columns_body(cy, vel, labels, rates, left, right):
    for out, y0 in ((left, 0), (right, cy - 2)):
        for k in range(2):
            cell = jnp.where(labels[:, y0 + k, :] == 1, rates[1], rates[0])
            out[:, FIELDS * k, :] = cell
            for f in range(3):
                out[:, FIELDS * k + f + 1, :] = vel[f, :, y0 + k, :]


def prep_body(cx, cy, level, vel, labels, rates, state, rate):
    def row(x, _):
        state[x, pl.ds(0, cy, stride=FIELDS), :] = level[x]
        for f in range(3):
            state[x, pl.ds(f + 1, cy, stride=FIELDS), :] = vel[f, x]
        cell = jnp.where(labels[x] == 1, rates[1], rates[0])
        for f in range(FIELDS):
            rate[x, pl.ds(f, cy, stride=FIELDS), :] = cell
        return 0

    lax.fori_loop(0, cx, row, 0)


def edge_rows_body(cx, pairs, mix, *refs):
    sources, (top, bot) = refs[:-2], refs[-2:]
    state, ym, yp = sources[0], sources[-2], sources[-1]
    wide = pairs + 2
    for out, rows in ((top, (0, 1)), (bot, (cx - 2, cx - 1))):
        for k, x in enumerate(rows):
            out[k * wide] = ym[x]
            out[k * wide + pairs + 1] = yp[x]
            for q in range(pairs):
                v = state[x * pairs + q]
                if mix:
                    v = jnp.where(sublane(v.shape) % FIELDS == 0, sources[1][x * pairs + q], v)
                out[k * wide + q + 1] = v


def weights_body(cx, cy, step, fraction, out):
    def row(x, _):
        for d in range(3):
            for k, w in enumerate(cubic_weights(fraction[step, d, x])):
                for f in range(FIELDS):
                    out[4 * d + k, x, pl.ds(f, cy, stride=FIELDS), :] = w
        return 0

    lax.fori_loop(0, cx, row, 0)


def fill_rows(pad, at, rows, pairs, own, ym, yp, change):
    wide = pairs + 2
    for n, x in enumerate(rows):
        pad[(at + n) * wide] = change(ym[x])
        pad[(at + n) * wide + pairs + 1] = change(yp[x])
        for q in range(pairs):
            pad[(at + n) * wide + q + 1] = own[x * pairs + q]


def spread_rate(v):
    v = jnp.where(sublane(v.shape) % FIELDS == 0, v, 0.0)
    v = v + turn(v, 1, 0)
    return v + turn(v, 2, 0)


def same(v):
    return v


def coef_row(pad, base, ax, yu, yd, zu, zd, c0, r, wide):
    shape = pad.shape[1:]
    half = sublane(shape) < FIELDS
    scale = jnp.where(sublane(shape) % FIELDS == 0, 0.0, 0.5)
    flipped = [turn(pad[base + j], FIELDS, 0) for j in range(wide)]
    for j in range(wide):
        own = pad[base + j]
        up = jnp.where(half, flipped[j], flipped[min(j + 1, wide - 1)])
        down = jnp.where(half, flipped[max(j - 1, 0)], flipped[j])
        at = r * wide + j
        cyu = (own + up) * scale
        cyd = (own + down) * scale
        czu = (own + turn(own, -1, 1)) * scale
        czd = (own + turn(own, 1, 1)) * scale
        yu[at] = cyu
        yd[at] = cyd
        zu[at] = czu
        zd[at] = czd
        c0[at] = 1.0 - (ax[at] + ax[at + wide] + cyu + cyd + czu + czd)


def face_row(pad, base, ax, r, wide):
    scale = jnp.where(sublane(pad.shape[1:]) % FIELDS == 0, 0.0, 0.5)
    for j in range(wide):
        ax[r * wide + j] = (pad[base - wide + j] + pad[base + j]) * scale


def coef_inner_body(cx, pairs, rate, ym, yp, ax, yu, yd, zu, zd, c0, pad):
    wide = pairs + 2

    def copy(x, _):
        pad[x * wide] = spread_rate(ym[x])
        pad[x * wide + pairs + 1] = spread_rate(yp[x])
        for q in range(pairs):
            pad[x * wide + q + 1] = rate[x * pairs + q]
        return 0

    lax.fori_loop(0, cx, copy, 0)

    def faces(r, _):
        face_row(pad, (r - 1) * wide, ax, r, wide)
        return 0

    lax.fori_loop(2, cx + 1, faces, 0)

    def row(r, _):
        coef_row(pad, (r - 1) * wide, ax, yu, yd, zu, zd, c0, r, wide)
        return 0

    lax.fori_loop(2, cx, row, 0)


def coef_outer_body(cx, pairs, rate, xm, xp, ym, yp, ax_inner, *refs):
    outs, pad = refs[:6], refs[6]
    ax, yu, yd, zu, zd, c0 = outs
    wide = pairs + 2
    outer_pad(pad, cx, pairs, rate, xm, xp, ym, yp, spread_rate)
    for half_at, faces in ((0, (0, 1)), (1, (4, 5))):
        base = 4 * half_at * wide
        for n in faces:
            face_row(pad, base + (1 + n - (3 if half_at else 0)) * wide, ax, n, wide)
    for j in range(wide):
        ax[2 * wide + j] = ax_inner[2 * wide + j]
        ax[3 * wide + j] = ax_inner[cx * wide + j]
    for n in range(2):
        coef_row(pad, (1 + n) * wide, ax, yu, yd, zu, zd, c0, n, wide)
    shifted = ax.at[pl.ds(wide, 5 * wide)]
    for n in range(2):
        coef_row(pad, (5 + n) * wide, shifted, yu, yd, zu, zd, c0, 2 + n, wide)


def outer_pad(pad, cx, pairs, own, xm, xp, ym, yp, change):
    wide = pairs + 2
    for k in range(2 * wide):
        pad[k] = change(xm[k])
        pad[6 * wide + k] = change(xp[k])
    fill_rows(pad, 2, (0, 1), pairs, own, ym, yp, change)
    fill_rows(pad, 4, (cx - 2, cx - 1), pairs, own, ym, yp, change)


def sweep_row(src, base, lo, hi, coefs, at, half):
    ax, yu, yd, zu, zd, c0, wide = coefs
    own = {j: src[base + j] for j in range(max(lo - 1, 0), min(hi + 1, wide))}
    flipped = {j: turn(v, FIELDS, 0) for j, v in own.items()}
    for j in range(lo, hi):
        up = jnp.where(half, flipped[j], flipped.get(j + 1, flipped[j]))
        down = jnp.where(half, flipped.get(j - 1, flipped[j]), flipped[j])
        v = own[j]
        k = at + j
        total = c0[k] * v + ax[k] * src[base - wide + j] + ax[k + wide] * src[base + wide + j]
        total = total + yu[k] * up + yd[k] * down
        total = total + zu[k] * turn(v, -1, 1) + zd[k] * turn(v, 1, 1)
        yield j, total


def lifts(shape):
    return jnp.where(sublane(shape) % FIELDS == 0, BUOYANCY, 0.0)


def diffuse_inner(cx, pairs, own, ym, yp, coefs, pad, mid, g):
    wide = pairs + 2
    half = sublane(pad.shape[1:]) < FIELDS
    lift = lifts(pad.shape[1:])
    coefs = tuple(coefs) + (wide,)

    def copy(x, _):
        pad[x * wide] = ym[x]
        pad[x * wide + pairs + 1] = yp[x]
        for q in range(pairs):
            pad[x * wide + q + 1] = own[x * pairs + q]
        return 0

    lax.fori_loop(0, cx, copy, 0)

    def first(x, _):
        for j, v in sweep_row(pad, x * wide, 0, wide, coefs, (x + 1) * wide, half):
            mid[x * wide + j] = v
        return 0

    lax.fori_loop(1, cx - 1, first, 0)

    def second(x, _):
        for j, v in sweep_row(mid, x * wide, 1, pairs + 1, coefs, (x + 1) * wide, half):
            g[x * pairs + j - 1] = v + lift * turn(v, -3, 0)
        return 0

    lax.fori_loop(2, cx - 2, second, 0)


def diffuse_outer(cx, pairs, own, xm, xp, ym, yp, coefs, outer, mid_inner, g_inner, pad, mid, g):
    wide = pairs + 2
    shape = pad.shape[1:]
    half = sublane(shape) < FIELDS
    lift = lifts(shape)
    zero = jnp.zeros(shape, jnp.float32)
    for k in range(3 * pairs):
        g[k] = zero
        g[(cx + 3) * pairs + k] = zero

    def copy(x, _):
        for q in range(pairs):
            g[(x + 3) * pairs + q] = g_inner[x * pairs + q]
        return 0

    lax.fori_loop(2, cx - 2, copy, 0)
    outer_pad(pad, cx, pairs, own, xm, xp, ym, yp, same)
    for j in range(wide):
        mid[2 * wide + j] = mid_inner[wide + j]
        mid[3 * wide + j] = mid_inner[2 * wide + j]
        mid[4 * wide + j] = mid_inner[(cx - 3) * wide + j]
        mid[5 * wide + j] = mid_inner[(cx - 2) * wide + j]
    low = tuple(outer) + (wide,)
    high = (outer[0].at[pl.ds(wide, 5 * wide)],) + tuple(outer[1:]) + (wide,)
    for n, (src, to, table) in enumerate(((1, 0, low), (2, 1, low), (5, 6, high), (6, 7, high))):
        lo, hi = (1, pairs + 1) if n in (0, 3) else (0, wide)
        for j, v in sweep_row(pad, src * wide, lo, hi, table, n * wide, half):
            mid[to * wide + j] = v
    inner = tuple(coefs) + (wide,)
    for src, x, table, at in (
        (1, 0, low, 1),
        (2, 1, inner, 2),
        (5, cx - 2, inner, cx - 1),
        (6, cx - 1, high, 2),
    ):
        for j, v in sweep_row(mid, src * wide, 1, pairs + 1, table, at * wide, half):
            g[(x + 3) * pairs + j - 1] = v + lift * turn(v, -3, 0)


def patch_row(g, w, cx, pairs, at, lead):
    shape = g.shape[1:]
    half = sublane(shape) < FIELDS
    rows = [(at + 1 - a + lead, jnp.clip(at + 1 - a, 0, cx - 1)) for a in range(4)]
    out = []
    zero = jnp.zeros(shape, jnp.float32)

    def finish(acc0, acc1, acc1_before):
        flipped = turn(acc1, FIELDS, 0) if acc1 is not None else zero
        flipped_before = turn(acc1_before, FIELDS, 0) if acc1_before is not None else zero
        value = jnp.where(half, flipped_before, flipped)
        return value if acc0 is None else acc0 + value

    p1 = p2 = p3 = p3_old = acc1_old = None
    for q in range(pairs):
        sums = [[None] * 4 for _ in range(4)]
        for a in range(4):
            padded, row = rows[a]
            k = pl.ds(SUB * q, SUB)
            h = g[padded * pairs + q] * w[a, row, k, :]
            wy = [w[4 + b, row, k, :] for b in range(4)]
            for c in range(4):
                hc = h * w[8 + c, row, k, :]
                for b in range(4):
                    t = hc * wy[b]
                    sums[b][c] = t if sums[b][c] is None else sums[b][c] + t
        p = []
        for b in range(4):
            s = sums[b]
            p.append((turn(s[0], -1, 1) + s[1]) + (turn(s[2], 1, 1) + turn(s[3], 2, 1)))
        acc1 = p[0] if p2 is None else p2 + p[0]
        acc0 = p1 if p3_old is None else p1 + p3_old
        out.append(finish(acc0, acc1, acc1_old))
        p3_old = p3
        p1, p2, p3 = p[1], p[2], p[3]
        acc1_old = acc1
    out.append(finish(p1 if p3_old is None else p1 + p3_old, p2, acc1_old))
    out.append(finish(p3, None, p2))
    return out


def spread(cx, pairs, rows_of, count, lead, g, w, shift_x, shift_y, step, own, right, left, far):
    shape = g.shape[1:]
    move_x = shift_x[0, 0, step]
    move_y = shift_y[0, 0, step]
    here = jnp.where(move_y == 0, 1.0, 0.0)
    up = jnp.where(move_y == 1, 1.0, 0.0)
    down = jnp.where(move_y == -1, 1.0, 0.0)

    def row(i, _):
        out = patch_row(g, w, cx, pairs, rows_of(i), lead)
        low, high = out[0], out[pairs + 1]
        for q in range(pairs):
            v = out[q + 1]
            o, r, l = v * here, v * up, v * down
            if q == 0:
                o = o + high * down
                r = r + high * here
            if q == pairs - 1:
                o = o + low * up
                l = l + low * here
            own[i * pairs + q] = o
            right[i * pairs + q] = r
            left[i * pairs + q] = l
        far[i] = high * up + low * down
        return 0

    lax.fori_loop(0, count, row, 0)
    mx = jnp.full(shape, move_x.astype(jnp.float32))
    right[count * pairs] = mx
    left[count * pairs] = mx
    far[count] = mx
    far[count + 1] = jnp.full(shape, move_y.astype(jnp.float32))


def inner_body(cx, pairs, step, rows_of, count, *refs):
    own, ym, yp, coefs, w, sx, sy = refs[0], refs[1], refs[2], refs[3:9], refs[9], refs[10], refs[11]
    o, r, l, far, mid, g, pad = refs[12:]
    diffuse_inner(cx, pairs, own, ym, yp, coefs, pad, mid, g)
    spread(cx, pairs, rows_of, count, 0, g, w, sx, sy, step, o, r, l, far)


def outer_body(cx, pairs, step, rows_of, count, *refs):
    own, halos, coefs, outer = refs[0], refs[1:5], refs[5:11], refs[11:17]
    mid_inner, g_inner, w, sx, sy = refs[17:22]
    o, r, l, far, pad, mid, g = refs[22:]
    diffuse_outer(cx, pairs, own, *halos, coefs, outer, mid_inner, g_inner, pad, mid, g)
    spread(cx, pairs, rows_of, count, 3, g, w, sx, sy, step, o, r, l, far)


def gather_body(pairs, step, main, rims, *refs):
    own, right, left, far_low, far_high, sx = refs[:6]
    outs = refs[6:11]
    shape = own.shape[1:]
    count = own.shape[0] // pairs
    skip = 3 if rims else 0
    mine = jnp.full(shape, sx[0, 0, step].astype(jnp.float32))
    moves = (mine, right[count * pairs], left[count * pairs])
    far_moves = (far_low[count], far_high[count])
    far_gates = (far_low[count + 1] == 1.0, far_high[count + 1] == -1.0)
    side = 2 * lax.rem(lax.axis_index("gx"), 2) - 1
    targets = (side, -side, 2 * side, -2 * side, jnp.int32(0))

    def hit(move, t):
        return jnp.where(move == t.astype(jnp.float32), 1.0, 0.0)

    def total(masks, fars, i, q):
        v = masks[0] * own[i * pairs + q] + masks[1] * right[i * pairs + q] + masks[2] * left[i * pairs + q]
        if q == 0:
            v = v + fars[0] * far_low[i]
        if q == pairs - 1:
            v = v + fars[1] * far_high[i]
        return v

    def masks_of(t):
        masks = [hit(m, t) for m in moves]
        fars = [jnp.where(gate, hit(m, t), 0.0) for gate, m in zip(far_gates, far_moves)]
        return masks, fars

    for out, t in zip(outs, targets):
        masks, fars = masks_of(t)

        def row(i, _, out=out, masks=masks, fars=fars):
            for q in range(pairs):
                out[i * pairs + q] = total(masks, fars, i + skip, q)
            return 0

        lax.fori_loop(0, main, row, 0)
        if rims:
            for source, row_at, step_to in ((0, 0, -1), (1, 1, -1), (2, main - 1, 1)):
                masks, fars = masks_of(t + step_to)
                for q in range(pairs):
                    out[row_at * pairs + q] = out[row_at * pairs + q] + total(masks, fars, source, q)
    if rims:
        high, low = refs[11:]
        masks, fars = masks_of(jnp.int32(2))
        for k in range(2):
            for q in range(pairs):
                high[k * pairs + q] = total(masks, fars, k, q)
        masks, fars = masks_of(jnp.int32(-2))
        for q in range(pairs):
            low[q] = total(masks, fars, 2, q)


def add_body(a, b, out):
    group = 8 if out.shape[0] % 8 == 0 else 1

    def rows(i, _):
        for j in range(group):
            out[i * group + j] = a[i * group + j] + b[i * group + j]
        return 0

    lax.fori_loop(0, out.shape[0] // group, rows, 0)


def merge(cx, pairs, chunks, parts, put):
    for runs, (t0, e0, f, d) in zip(chunks, (parts[0:4], parts[4:8])):
        for local, base, rows in runs:

            def row(i, _, t0=t0, e0=e0, f=f, d=d, local=local, base=base):
                for q in range(pairs):
                    at = (i + local) * pairs + q
                    put(i + base, q, (t0[at] + e0[at]) + (f[at] + d[at]), False)
                return 0

            lax.fori_loop(0, rows, row, 0)
    high, low = parts[8:10]
    for q in range(pairs):
        for k in range(2):
            put(k, q, high[k * pairs + q], True)
        put(cx - 1, q, low[q], True)


def merge_body(cx, pairs, chunks, *refs):
    parts = refs[:10]
    out, left, right = refs[10:]

    def put(x, q, v, add):
        at = x * pairs + q
        out[at] = out[at] + v if add else v

    merge(cx, pairs, chunks, parts, put)
    for x in range(cx):
        left[x] = out[x * pairs]
        right[x] = out[x * pairs + pairs - 1]


def finish_body(cx, cy, pairs, chunks, *refs):
    parts = refs[:10]
    level, vel, out = refs[10:]

    def put(x, q, v, add):
        at = pl.ds(SUB * q, SUB)
        out[x, at, :] = out[x, at, :] + v if add else v

    merge(cx, pairs, chunks, parts, put)

    def row(x, _):
        level[x] = out[x, pl.ds(0, cy, stride=FIELDS), :]
        for f in range(3):
            vel[f, x] = out[x, pl.ds(f + 1, cy, stride=FIELDS), :]
        return 0

    lax.fori_loop(0, cx, row, 0)


def moved(value, axis, steps):
    count = lax.axis_size(axis)
    return lax.ppermute(value, axis, [(i, (i + steps) % count) for i in range(count)])


def swapped(value):
    return lax.ppermute(value, "gx", [(i, i ^ 1) for i in range(lax.axis_size("gx"))])


def crossed(value, sign):
    count = lax.axis_size("gx")
    return lax.ppermute(
        value, "gx", [(i, (i + (2 if i % 2 else -2) * sign) % count) for i in range(count)]
    )


def on_device(level, vel, fraction, shift_x, shift_y, labels, rates):
    cx, cy, cz = level.shape
    pairs = cy // 2
    wide = pairs + 2
    ny = lax.axis_size("gy")

    def plane(n):
        return f32(n, SUB, cz)

    def scratch(n):
        return pltpu.VMEM((n, SUB, cz), jnp.float32)

    left, right = call(
        functools.partial(columns_body, cy),
        [plane(cx)] * 2,
        (vel, labels, rates),
        [VMEM, VMEM, SMEM],
    )
    state, rate = call(
        functools.partial(prep_body, cx, cy),
        [f32(cx, FIELDS * cy, cz)] * 2,
        (level, vel, labels, rates),
        [VMEM, VMEM, VMEM, SMEM],
    )
    state = state.reshape(cx * pairs, SUB, cz)
    rate = rate.reshape(cx * pairs, SUB, cz)
    weights = [
        call(
            functools.partial(weights_body, cx, cy, s),
            [f32(12, cx, FIELDS * cy, cz)],
            (fraction,),
            [VMEM],
        )[0]
        for s in range(STEPS)
    ]
    coefs = outer = None

    inner = 4
    count_a = cx - 2 * inner + 1
    main = (count_a, cx - count_a)
    chunk_runs = (
        ((0, inner, count_a),),
        ((0, 0, inner), (inner, inner + count_a, cx - inner - count_a)),
    )

    def rows_a(i):
        return i + inner

    def rows_b(i):
        k = i - 3
        body = jnp.where(k < inner, k, k + count_a)
        return jnp.where(i < 2, cx + i, jnp.where(i < 3, -1, body))

    counts = (main[0], main[1] + 3)

    def outs(n):
        return [plane(n * pairs), plane(n * pairs + 1), plane(n * pairs + 1), plane(n + 2)]

    for step in range(STEPS - 1, -1, -1):
        first = coefs is None
        ym = moved(right, "gy", 1)
        yp = moved(left, "gy", -1)
        states = (state, rate) if first else (state,)
        top, bot = call(
            functools.partial(edge_rows_body, cx, pairs, first),
            [plane(2 * wide)] * 2,
            (*states, ym, yp),
            [VMEM] * (len(states) + 2),
        )
        xm = moved(bot, "gx", 1)
        xp = moved(top, "gx", -1)
        if first:
            coefs = call(
                functools.partial(coef_inner_body, cx, pairs),
                [plane((cx + 3) * wide)] + [plane((cx + 2) * wide)] * 5,
                (rate, ym, yp),
                [VMEM] * 3,
                [scratch(cx * wide)],
            )
        *sent_a, mid, g = call(
            functools.partial(inner_body, cx, pairs, step, rows_a, counts[0]),
            outs(counts[0]) + [plane(cx * wide), plane(cx * pairs)],
            (state, ym, yp, *coefs, weights[step], shift_x, shift_y),
            [VMEM] * 10 + [SMEM] * 2,
            [scratch(cx * wide)],
            flops=20000000,
        )
        if first:
            outer = call(
                functools.partial(coef_outer_body, cx, pairs),
                [plane(6 * wide)] + [plane(4 * wide)] * 5,
                (rate, xm, xp, ym, yp, coefs[0]),
                [VMEM] * 6,
                [scratch(8 * wide)],
            )
        sent_b = call(
            functools.partial(outer_body, cx, pairs, step, rows_b, counts[1]),
            outs(counts[1]),
            (state, xm, xp, ym, yp, *coefs, *outer, mid, g, weights[step], shift_x, shift_y),
            [VMEM] * 20 + [SMEM] * 2,
            [scratch(8 * wide), scratch(8 * wide), scratch((cx + 6) * pairs)],
            flops=10000000,
        )
        chunks = []
        for n, (own, right, left, far) in enumerate((sent_a, sent_b)):
            if n:
                own, _ = lax.optimization_barrier((own, chunks[0]))
            right = moved(right, "gy", 1)
            left = moved(left, "gy", -1)
            far_low = moved(far, "gy", 2)
            far_high = far_low if ny == 4 else moved(far, "gy", -2)
            e1, e0, f, k, t0, *rims = call(
                functools.partial(gather_body, pairs, step, main[n], n == 1),
                [plane(main[n] * pairs)] * 5 + ([plane(2 * pairs), plane(pairs)] if n else []),
                (own, right, left, far_low, far_high, shift_x),
                [VMEM] * 5 + [SMEM],
                flops=3000000,
            )
            e1 = swapped(e1)
            f = crossed(f, 1)
            e0 = swapped(e0)
            (d,) = call(add_body, [plane(main[n] * pairs)], (k, e1), [VMEM] * 2)
            d = crossed(d, -1)
            chunks += [t0, e0, f, d]
        high, low = rims
        high = moved(high, "gx", 3)
        low = moved(low, "gx", -3)
        chunks += [high, low]
        if step:
            state, left, right = call(
                functools.partial(merge_body, cx, pairs, chunk_runs),
                [plane(cx * pairs)] + [plane(cx)] * 2,
                chunks,
                [VMEM] * 10,
            )
        else:
            return call(
                functools.partial(finish_body, cx, cy, pairs, chunk_runs),
                [f32(cx, cy, cz), f32(3, cx, cy, cz)],
                chunks,
                [VMEM] * 10,
                [pltpu.VMEM((cx, FIELDS * cy, cz), jnp.float32)],
            )


def solution(mesh):
    in_specs = (
        P("gx", "gy", None),
        P(None, "gx", "gy", None),
        P(None, None, "gx", "gy", None),
        P("gx", "gy", None),
        P("gx", "gy", None),
        P("gx", "gy", None),
        P(),
    )
    out_specs = (P("gx", "gy", None), P(None, "gx", "gy", None))
    return jax.shard_map(
        on_device, mesh=mesh, in_specs=in_specs, out_specs=out_specs, check_vma=False
    )
```

```python
import functools

import jax
import jax.numpy as jnp
from jax import lax
from jax.experimental import pallas as pl
from jax.experimental.pallas import tpu as pltpu
from jax.sharding import PartitionSpec as P


STEPS = 2
BUOYANCY = 0.8
FIELDS = 4
SUB = 8
VMEM = pl.BlockSpec(memory_space=pltpu.VMEM)
SMEM = pl.BlockSpec(memory_space=pltpu.SMEM)


def call(body, outs, args, specs, scratch=(), flops=1000000):
    moved = sum(a.size for a in args) * 4 + sum(o.size for o in outs) * 4
    return pl.pallas_call(
        body,
        out_shape=tuple(outs),
        in_specs=list(specs),
        out_specs=tuple(VMEM for _ in outs),
        scratch_shapes=list(scratch),
        compiler_params=pltpu.CompilerParams(vmem_limit_bytes=8 * 1024 * 1024),
        cost_estimate=pl.CostEstimate(flops=flops, bytes_accessed=moved, transcendentals=0),
    )(*args)


def f32(*shape):
    return jax.ShapeDtypeStruct(shape, jnp.float32)


def sublane(shape):
    return lax.broadcasted_iota(jnp.int32, shape, 0)


def turn(v, steps, axis):
    return pltpu.roll(v, steps % v.shape[axis], axis)


def cubic_weights(position):
    squared = position * position
    cubed = squared * position
    return (
        (2.0 * squared - cubed - position) * 0.5,
        (3.0 * cubed - 5.0 * squared + 2.0) * 0.5,
        (4.0 * squared - 3.0 * cubed + position) * 0.5,
        (cubed - squared) * 0.5,
    )


def columns_body(cy, vel, labels, rates_at, left, right, near_vel, near_labels, rates, sem):
    copies = [pltpu.make_async_copy(rates_at, rates, sem.at[4])]
    for n, y0 in enumerate((0, cy - 2)):
        at = pl.ds(y0, 2)
        copies.append(pltpu.make_async_copy(vel.at[:, :, at, :], near_vel.at[n], sem.at[2 * n]))
        copies.append(pltpu.make_async_copy(labels.at[:, at, :], near_labels.at[n], sem.at[2 * n + 1]))
    for copy in copies:
        copy.start()
    for copy in copies:
        copy.wait()
    for n, out in enumerate((left, right)):
        for k in range(2):
            cell = jnp.where(near_labels[n, :, k, :] == 1, rates[1], rates[0])
            out[:, FIELDS * k, :] = cell
            for f in range(3):
                out[:, FIELDS * k + f + 1, :] = near_vel[n, f, :, k, :]


def in_hbm(value):
    return pltpu.with_memory_space_constraint(value, pltpu.HBM)


def prep_body(cx, cy, step, *refs):
    level_at, vel_at, labels_at, rates_at, sx_at, sy_at, fraction = refs[:7]
    state, rate, weights, own_moves = refs[7:11]
    level, vel, labels, rates, sx, sy, near, sem = refs[11:]
    copies = [
        pltpu.make_async_copy(a, b, sem.at[n])
        for n, (a, b) in enumerate(
            zip(
                (vel_at, level_at, labels_at, rates_at, sx_at, sy_at, fraction.at[step]),
                (vel, level, labels, rates, sx, sy, near),
            )
        )
    ]
    for copy in copies:
        copy.start()
    for copy in copies[:6]:
        copy.wait()
    for n in range(STEPS):
        own_moves[n] = jnp.full(own_moves.shape[1:], sx[0, 0, n].astype(jnp.float32))
        own_moves[STEPS + n] = jnp.full(own_moves.shape[1:], sy[0, 0, n].astype(jnp.float32))

    def row(x, _):
        state[x, pl.ds(0, cy, stride=FIELDS), :] = level[x]
        for f in range(3):
            state[x, pl.ds(f + 1, cy, stride=FIELDS), :] = vel[f, x]
        cell = jnp.where(labels[x] == 1, rates[1], rates[0])
        for f in range(FIELDS):
            rate[x, pl.ds(f, cy, stride=FIELDS), :] = cell
        return 0

    lax.fori_loop(0, cx, row, 0)
    copies[6].wait()
    fill_weights(cx, cy, near, weights)


def edge_rows_body(cx, pairs, mix, *refs):
    sources, (top, bot) = refs[:-2], refs[-2:]
    state, ym, yp = sources[0], sources[-2], sources[-1]
    wide = pairs + 2
    for out, rows in ((top, (0, 1)), (bot, (cx - 2, cx - 1))):
        for k, x in enumerate(rows):
            out[k * wide] = ym[x]
            out[k * wide + pairs + 1] = yp[x]
            for q in range(pairs):
                v = state[x * pairs + q]
                if mix:
                    v = jnp.where(sublane(v.shape) % FIELDS == 0, sources[1][x * pairs + q], v)
                out[k * wide + q + 1] = v


def fill_weights(cx, cy, near, out):
    pairs = cy // 2

    def row(x, _):
        for d in range(3):
            for k, w in enumerate(cubic_weights(near[d, x])):
                table = out.at[4 * d + k, pl.ds(x * pairs, pairs)].reshape(FIELDS * cy, w.shape[-1])
                for f in range(FIELDS):
                    table[pl.ds(f, cy, stride=FIELDS), :] = w
        return 0

    lax.fori_loop(0, cx, row, 0)


def weights_body(cx, cy, step, fraction, out, near, sem):
    copy = pltpu.make_async_copy(fraction.at[step], near, sem)
    copy.start()
    copy.wait()
    fill_weights(cx, cy, near, out)


def fill_rows(pad, at, rows, pairs, own, ym, yp, change):
    wide = pairs + 2
    for n, x in enumerate(rows):
        pad[(at + n) * wide] = change(ym[x])
        pad[(at + n) * wide + pairs + 1] = change(yp[x])
        for q in range(pairs):
            pad[(at + n) * wide + q + 1] = own[x * pairs + q]


def spread_rate(v):
    v = jnp.where(sublane(v.shape) % FIELDS == 0, v, 0.0)
    v = v + turn(v, 1, 0)
    return v + turn(v, 2, 0)


def same(v):
    return v


def coef_row(pad, base, ax, yu, yd, zu, zd, c0, r, wide):
    shape = pad.shape[1:]
    half = sublane(shape) < FIELDS
    scale = jnp.where(sublane(shape) % FIELDS == 0, 0.0, 0.5)
    flipped = [turn(pad[base + j], FIELDS, 0) for j in range(wide)]
    for j in range(wide):
        own = pad[base + j]
        up = jnp.where(half, flipped[j], flipped[min(j + 1, wide - 1)])
        down = jnp.where(half, flipped[max(j - 1, 0)], flipped[j])
        at = r * wide + j
        cyu = (own + up) * scale
        cyd = (own + down) * scale
        czu = (own + turn(own, -1, 1)) * scale
        czd = (own + turn(own, 1, 1)) * scale
        yu[at] = cyu
        yd[at] = cyd
        zu[at] = czu
        zd[at] = czd
        c0[at] = 1.0 - (ax[at] + ax[at + wide] + cyu + cyd + czu + czd)


def face_row(pad, base, ax, r, wide):
    scale = jnp.where(sublane(pad.shape[1:]) % FIELDS == 0, 0.0, 0.5)
    for j in range(wide):
        ax[r * wide + j] = (pad[base - wide + j] + pad[base + j]) * scale


def coef_inner_body(cx, pairs, rate, ym, yp, ax, yu, yd, zu, zd, c0, pad):
    wide = pairs + 2

    def copy(x, _):
        pad[x * wide] = spread_rate(ym[x])
        pad[x * wide + pairs + 1] = spread_rate(yp[x])
        for q in range(pairs):
            pad[x * wide + q + 1] = rate[x * pairs + q]
        return 0

    lax.fori_loop(0, cx, copy, 0)

    def faces(r, _):
        face_row(pad, (r - 1) * wide, ax, r, wide)
        return 0

    lax.fori_loop(2, cx + 1, faces, 0)

    def row(r, _):
        coef_row(pad, (r - 1) * wide, ax, yu, yd, zu, zd, c0, r, wide)
        return 0

    lax.fori_loop(2, cx, row, 0)


def coef_outer_body(cx, pairs, rate, xm, xp, ym, yp, ax_inner, *refs):
    outs, pad = refs[:6], refs[6]
    ax, yu, yd, zu, zd, c0 = outs
    wide = pairs + 2
    outer_pad(pad, cx, pairs, rate, xm, xp, ym, yp, spread_rate)
    for half_at, faces in ((0, (0, 1)), (1, (4, 5))):
        base = 4 * half_at * wide
        for n in faces:
            face_row(pad, base + (1 + n - (3 if half_at else 0)) * wide, ax, n, wide)
    for j in range(wide):
        ax[2 * wide + j] = ax_inner[2 * wide + j]
        ax[3 * wide + j] = ax_inner[cx * wide + j]
    for n in range(2):
        coef_row(pad, (1 + n) * wide, ax, yu, yd, zu, zd, c0, n, wide)
    shifted = ax.at[pl.ds(wide, 5 * wide)]
    for n in range(2):
        coef_row(pad, (5 + n) * wide, shifted, yu, yd, zu, zd, c0, 2 + n, wide)


def outer_pad(pad, cx, pairs, own, xm, xp, ym, yp, change):
    wide = pairs + 2
    for k in range(2 * wide):
        pad[k] = change(xm[k])
        pad[6 * wide + k] = change(xp[k])
    fill_rows(pad, 2, (0, 1), pairs, own, ym, yp, change)
    fill_rows(pad, 4, (cx - 2, cx - 1), pairs, own, ym, yp, change)


def sweep_row(src, base, lo, hi, coefs, at, half):
    ax, yu, yd, zu, zd, c0, wide = coefs
    own = {j: src[base + j] for j in range(max(lo - 1, 0), min(hi + 1, wide))}
    flipped = {j: turn(v, FIELDS, 0) for j, v in own.items()}
    for j in range(lo, hi):
        up = jnp.where(half, flipped[j], flipped.get(j + 1, flipped[j]))
        down = jnp.where(half, flipped.get(j - 1, flipped[j]), flipped[j])
        v = own[j]
        k = at + j
        total = c0[k] * v + ax[k] * src[base - wide + j] + ax[k + wide] * src[base + wide + j]
        total = total + yu[k] * up + yd[k] * down
        total = total + zu[k] * turn(v, -1, 1) + zd[k] * turn(v, 1, 1)
        yield j, total


def lifts(shape):
    return jnp.where(sublane(shape) % FIELDS == 0, BUOYANCY, 0.0)


def diffuse_inner(cx, pairs, own, ym, yp, coefs, pad, mid, g):
    wide = pairs + 2
    half = sublane(pad.shape[1:]) < FIELDS
    lift = lifts(pad.shape[1:])
    coefs = tuple(coefs) + (wide,)

    def copy(x, _):
        pad[x * wide] = ym[x]
        pad[x * wide + pairs + 1] = yp[x]
        for q in range(pairs):
            pad[x * wide + q + 1] = own[x * pairs + q]
        return 0

    lax.fori_loop(0, cx, copy, 0)

    def first(x, _):
        for j, v in sweep_row(pad, x * wide, 0, wide, coefs, (x + 1) * wide, half):
            mid[x * wide + j] = v
        return 0

    lax.fori_loop(1, cx - 1, first, 0)

    def second(x, _):
        for j, v in sweep_row(mid, x * wide, 1, pairs + 1, coefs, (x + 1) * wide, half):
            g[x * pairs + j - 1] = v + lift * turn(v, -3, 0)
        return 0

    lax.fori_loop(2, cx - 2, second, 0)


def diffuse_outer(cx, pairs, own, xm, xp, ym, yp, coefs, outer, mid_inner, g_inner, pad, mid, g):
    wide = pairs + 2
    shape = pad.shape[1:]
    half = sublane(shape) < FIELDS
    lift = lifts(shape)
    zero = jnp.zeros(shape, jnp.float32)
    for k in range(3 * pairs):
        g[k] = zero
        g[(cx + 3) * pairs + k] = zero

    def copy(x, _):
        for q in range(pairs):
            g[(x + 3) * pairs + q] = g_inner[x * pairs + q]
        return 0

    lax.fori_loop(2, cx - 2, copy, 0)
    outer_pad(pad, cx, pairs, own, xm, xp, ym, yp, same)
    for j in range(wide):
        mid[2 * wide + j] = mid_inner[wide + j]
        mid[3 * wide + j] = mid_inner[2 * wide + j]
        mid[4 * wide + j] = mid_inner[(cx - 3) * wide + j]
        mid[5 * wide + j] = mid_inner[(cx - 2) * wide + j]
    low = tuple(outer) + (wide,)
    high = (outer[0].at[pl.ds(wide, 5 * wide)],) + tuple(outer[1:]) + (wide,)
    for n, (src, to, table) in enumerate(((1, 0, low), (2, 1, low), (5, 6, high), (6, 7, high))):
        lo, hi = (1, pairs + 1) if n in (0, 3) else (0, wide)
        for j, v in sweep_row(pad, src * wide, lo, hi, table, n * wide, half):
            mid[to * wide + j] = v
    inner = tuple(coefs) + (wide,)
    for src, x, table, at in (
        (1, 0, low, 1),
        (2, 1, inner, 2),
        (5, cx - 2, inner, cx - 1),
        (6, cx - 1, high, 2),
    ):
        for j, v in sweep_row(mid, src * wide, 1, pairs + 1, table, at * wide, half):
            g[(x + 3) * pairs + j - 1] = v + lift * turn(v, -3, 0)


def patch_row(g, w, cx, pairs, at, lead):
    shape = g.shape[1:]
    half = sublane(shape) < FIELDS
    rows = [(at + 1 - a + lead, jnp.clip(at + 1 - a, 0, cx - 1)) for a in range(4)]
    out = []
    zero = jnp.zeros(shape, jnp.float32)

    def finish(acc0, acc1, acc1_before):
        flipped = turn(acc1, FIELDS, 0) if acc1 is not None else zero
        flipped_before = turn(acc1_before, FIELDS, 0) if acc1_before is not None else zero
        value = jnp.where(half, flipped_before, flipped)
        return value if acc0 is None else acc0 + value

    p1 = p2 = p3 = p3_old = acc1_old = None
    for q in range(pairs):
        sums = [[None] * 4 for _ in range(4)]
        for a in range(4):
            padded, row = rows[a]
            k = row * pairs + q
            h = g[padded * pairs + q] * w[a, k]
            wy = [w[4 + b, k] for b in range(4)]
            for c in range(4):
                hc = h * w[8 + c, k]
                for b in range(4):
                    t = hc * wy[b]
                    sums[b][c] = t if sums[b][c] is None else sums[b][c] + t
        p = []
        for b in range(4):
            s = sums[b]
            p.append((turn(s[0], -1, 1) + s[1]) + (turn(s[2], 1, 1) + turn(s[3], 2, 1)))
        acc1 = p[0] if p2 is None else p2 + p[0]
        acc0 = p1 if p3_old is None else p1 + p3_old
        out.append(finish(acc0, acc1, acc1_old))
        p3_old = p3
        p1, p2, p3 = p[1], p[2], p[3]
        acc1_old = acc1
    out.append(finish(p1 if p3_old is None else p1 + p3_old, p2, acc1_old))
    out.append(finish(p3, None, p2))
    return out


def spread(cx, pairs, rows_of, count, lead, g, w, moves, step, own, right, left, far):
    move_x = moves[step]
    move_y = moves[STEPS + step]
    here = jnp.where(move_y == 0, 1.0, 0.0)
    up = jnp.where(move_y == 1, 1.0, 0.0)
    down = jnp.where(move_y == -1, 1.0, 0.0)

    def row(i, _):
        out = patch_row(g, w, cx, pairs, rows_of(i), lead)
        low, high = out[0], out[pairs + 1]
        for q in range(pairs):
            v = out[q + 1]
            o, r, l = v * here, v * up, v * down
            if q == 0:
                o = o + high * down
                r = r + high * here
            if q == pairs - 1:
                o = o + low * up
                l = l + low * here
            own[i * pairs + q] = o
            right[i * pairs + q] = r
            left[i * pairs + q] = l
        far[i] = high * up + low * down
        return 0

    lax.fori_loop(0, count, row, 0)
    right[count * pairs] = move_x
    left[count * pairs] = move_x
    far[count] = move_x
    far[count + 1] = move_y


def inner_body(cx, pairs, step, rows_of, count, *refs):
    own, ym, yp, coefs, w, moves = refs[0], refs[1], refs[2], refs[3:9], refs[9], refs[10]
    o, r, l, far, mid, g, pad = refs[11:]
    diffuse_inner(cx, pairs, own, ym, yp, coefs, pad, mid, g)
    spread(cx, pairs, rows_of, count, 0, g, w, moves, step, o, r, l, far)


def outer_body(cx, pairs, step, rows_of, count, *refs):
    own, halos, coefs, outer = refs[0], refs[1:5], refs[5:11], refs[11:17]
    mid_inner, g_inner, w, moves = refs[17:21]
    o, r, l, far, pad, mid, g = refs[21:]
    diffuse_outer(cx, pairs, own, *halos, coefs, outer, mid_inner, g_inner, pad, mid, g)
    spread(cx, pairs, rows_of, count, 3, g, w, moves, step, o, r, l, far)


def gather_body(pairs, step, main, rims, *refs):
    own, right, left, far_low, far_high, own_moves = refs[:6]
    outs = refs[6:11]
    count = own.shape[0] // pairs
    skip = 3 if rims else 0
    mine = own_moves[step]
    moves = (mine, right[count * pairs], left[count * pairs])
    far_moves = (far_low[count], far_high[count])
    far_gates = (far_low[count + 1] == 1.0, far_high[count + 1] == -1.0)
    side = 2 * lax.rem(lax.axis_index("gx"), 2) - 1
    targets = (side, -side, 2 * side, -2 * side, jnp.int32(0))

    def hit(move, t):
        return jnp.where(move == t.astype(jnp.float32), 1.0, 0.0)

    def total(masks, fars, i, q):
        v = masks[0] * own[i * pairs + q] + masks[1] * right[i * pairs + q] + masks[2] * left[i * pairs + q]
        if q == 0:
            v = v + fars[0] * far_low[i]
        if q == pairs - 1:
            v = v + fars[1] * far_high[i]
        return v

    def masks_of(t):
        masks = [hit(m, t) for m in moves]
        fars = [jnp.where(gate, hit(m, t), 0.0) for gate, m in zip(far_gates, far_moves)]
        return masks, fars

    for out, t in zip(outs, targets):
        masks, fars = masks_of(t)

        def row(i, _, out=out, masks=masks, fars=fars):
            for q in range(pairs):
                out[i * pairs + q] = total(masks, fars, i + skip, q)
            return 0

        lax.fori_loop(0, main, row, 0)
        if rims:
            for source, row_at, step_to in ((0, 0, -1), (1, 1, -1), (2, main - 1, 1)):
                masks, fars = masks_of(t + step_to)
                for q in range(pairs):
                    out[row_at * pairs + q] = out[row_at * pairs + q] + total(masks, fars, source, q)
    if rims:
        high, low = refs[11:]
        masks, fars = masks_of(jnp.int32(2))
        for k in range(2):
            for q in range(pairs):
                high[k * pairs + q] = total(masks, fars, k, q)
        masks, fars = masks_of(jnp.int32(-2))
        for q in range(pairs):
            low[q] = total(masks, fars, 2, q)


def add_body(a, b, out):
    group = 8 if out.shape[0] % 8 == 0 else 1

    def rows(i, _):
        for j in range(group):
            out[i * group + j] = a[i * group + j] + b[i * group + j]
        return 0

    lax.fori_loop(0, out.shape[0] // group, rows, 0)


def merge(cx, pairs, chunks, parts, put):
    for runs, (t0, e0, f, d) in zip(chunks, (parts[0:4], parts[4:8])):
        for local, base, rows in runs:

            def row(i, _, t0=t0, e0=e0, f=f, d=d, local=local, base=base):
                for q in range(pairs):
                    at = (i + local) * pairs + q
                    put(i + base, q, (t0[at] + e0[at]) + (f[at] + d[at]), False)
                return 0

            lax.fori_loop(0, rows, row, 0)
    high, low = parts[8:10]
    for q in range(pairs):
        for k in range(2):
            put(k, q, high[k * pairs + q], True)
        put(cx - 1, q, low[q], True)


def merge_body(cx, pairs, chunks, *refs):
    parts = refs[:10]
    out, left, right = refs[10:]

    def put(x, q, v, add):
        at = x * pairs + q
        out[at] = out[at] + v if add else v

    merge(cx, pairs, chunks, parts, put)
    for x in range(cx):
        left[x] = out[x * pairs]
        right[x] = out[x * pairs + pairs - 1]


def finish_body(cx, cy, pairs, chunks, *refs):
    parts = refs[:10]
    level, vel, out = refs[10:]

    def put(x, q, v, add):
        at = pl.ds(SUB * q, SUB)
        out[x, at, :] = out[x, at, :] + v if add else v

    merge(cx, pairs, chunks, parts, put)

    def row(x, _):
        level[x] = out[x, pl.ds(0, cy, stride=FIELDS), :]
        for f in range(3):
            vel[f, x] = out[x, pl.ds(f + 1, cy, stride=FIELDS), :]
        return 0

    lax.fori_loop(0, cx, row, 0)


def moved(value, axis, steps):
    count = lax.axis_size(axis)
    return lax.ppermute(value, axis, [(i, (i + steps) % count) for i in range(count)])


def swapped(value):
    return lax.ppermute(value, "gx", [(i, i ^ 1) for i in range(lax.axis_size("gx"))])


def crossed(value, sign):
    count = lax.axis_size("gx")
    return lax.ppermute(
        value, "gx", [(i, (i + (2 if i % 2 else -2) * sign) % count) for i in range(count)]
    )


def on_device(level, vel, fraction, shift_x, shift_y, labels, rates):
    cx, cy, cz = level.shape
    pairs = cy // 2
    wide = pairs + 2
    ny = lax.axis_size("gy")

    def plane(n):
        return f32(n, SUB, cz)

    def scratch(n):
        return pltpu.VMEM((n, SUB, cz), jnp.float32)

    level, vel, labels, rates = map(in_hbm, (level, vel, labels, rates))
    fraction, shift_x, shift_y = map(in_hbm, (fraction, shift_x, shift_y))
    hbm = pl.BlockSpec(memory_space=pltpu.HBM)
    rates_here = pltpu.SMEM(rates.shape, rates.dtype)
    near = pltpu.VMEM(fraction.shape[1:], fraction.dtype)
    left, right = call(
        functools.partial(columns_body, cy),
        [plane(cx)] * 2,
        (vel, labels, rates),
        [hbm] * 3,
        [
            pltpu.VMEM((2, *vel.shape[:2], 2, cz), vel.dtype),
            pltpu.VMEM((2, cx, 2, cz), labels.dtype),
            rates_here,
            pltpu.SemaphoreType.DMA((5,)),
        ],
    )
    last = STEPS - 1
    table = f32(12, cx * pairs + 1, SUB, cz)
    state, rate, weights_last, own_moves = call(
        functools.partial(prep_body, cx, cy, last),
        [f32(cx, FIELDS * cy, cz)] * 2 + [table, plane(2 * STEPS)],
        (level, vel, labels, rates, shift_x, shift_y, fraction),
        [hbm] * 7,
        [pltpu.VMEM(a.shape, a.dtype) for a in (level, vel, labels)]
        + [pltpu.SMEM(a.shape, a.dtype) for a in (rates, shift_x, shift_y)]
        + [near, pltpu.SemaphoreType.DMA((7,))],
    )
    state = state.reshape(cx * pairs, SUB, cz)
    rate = rate.reshape(cx * pairs, SUB, cz)
    weights = [
        call(
            functools.partial(weights_body, cx, cy, s),
            [table],
            (fraction,),
            [hbm],
            [near, pltpu.SemaphoreType.DMA],
        )[0]
        for s in range(last)
    ] + [weights_last]
    coefs = outer = None

    inner = 4
    count_a = cx - 2 * inner + 1
    main = (count_a, cx - count_a)
    chunk_runs = (
        ((0, inner, count_a),),
        ((0, 0, inner), (inner, inner + count_a, cx - inner - count_a)),
    )

    def rows_a(i):
        return i + inner

    def rows_b(i):
        k = i - 3
        body = jnp.where(k < inner, k, k + count_a)
        return jnp.where(i < 2, cx + i, jnp.where(i < 3, -1, body))

    counts = (main[0], main[1] + 3)

    def outs(n):
        return [plane(n * pairs), plane(n * pairs + 1), plane(n * pairs + 1), plane(n + 2)]

    for step in range(STEPS - 1, -1, -1):
        first = coefs is None
        ym = moved(right, "gy", 1)
        yp = moved(left, "gy", -1)
        states = (state, rate) if first else (state,)
        top, bot = call(
            functools.partial(edge_rows_body, cx, pairs, first),
            [plane(2 * wide)] * 2,
            (*states, ym, yp),
            [VMEM] * (len(states) + 2),
        )
        xm = moved(bot, "gx", 1)
        xp = moved(top, "gx", -1)
        if first:
            coefs = call(
                functools.partial(coef_inner_body, cx, pairs),
                [plane((cx + 3) * wide)] + [plane((cx + 2) * wide)] * 5,
                (rate, ym, yp),
                [VMEM] * 3,
                [scratch(cx * wide)],
            )
        *sent_a, mid, g = call(
            functools.partial(inner_body, cx, pairs, step, rows_a, counts[0]),
            outs(counts[0]) + [plane(cx * wide), plane(cx * pairs)],
            (state, ym, yp, *coefs, weights[step], own_moves),
            [VMEM] * 11,
            [scratch(cx * wide)],
            flops=20000000,
        )
        if first:
            outer = call(
                functools.partial(coef_outer_body, cx, pairs),
                [plane(6 * wide)] + [plane(4 * wide)] * 5,
                (rate, xm, xp, ym, yp, coefs[0]),
                [VMEM] * 6,
                [scratch(8 * wide)],
            )
        sent_b = call(
            functools.partial(outer_body, cx, pairs, step, rows_b, counts[1]),
            outs(counts[1]),
            (state, xm, xp, ym, yp, *coefs, *outer, mid, g, weights[step], own_moves),
            [VMEM] * 21,
            [scratch(8 * wide), scratch(8 * wide), scratch((cx + 6) * pairs)],
            flops=10000000,
        )
        chunks = []
        for n, (own, right, left, far) in enumerate((sent_a, sent_b)):
            if n:
                own, _ = lax.optimization_barrier((own, chunks[0]))
            right = moved(right, "gy", 1)
            left = moved(left, "gy", -1)
            far_low = moved(far, "gy", 2)
            far_high = far_low if ny == 4 else moved(far, "gy", -2)
            e1, e0, f, k, t0, *rims = call(
                functools.partial(gather_body, pairs, step, main[n], n == 1),
                [plane(main[n] * pairs)] * 5 + ([plane(2 * pairs), plane(pairs)] if n else []),
                (own, right, left, far_low, far_high, own_moves),
                [VMEM] * 6,
                flops=3000000,
            )
            e1 = swapped(e1)
            f = crossed(f, 1)
            e0 = swapped(e0)
            (d,) = call(add_body, [plane(main[n] * pairs)], (k, e1), [VMEM] * 2)
            d = crossed(d, -1)
            chunks += [t0, e0, f, d]
        high, low = rims
        high = moved(high, "gx", 3)
        low = moved(low, "gx", -3)
        chunks += [high, low]
        if step:
            state, left, right = call(
                functools.partial(merge_body, cx, pairs, chunk_runs),
                [plane(cx * pairs)] + [plane(cx)] * 2,
                chunks,
                [VMEM] * 10,
            )
        else:
            return call(
                functools.partial(finish_body, cx, cy, pairs, chunk_runs),
                [f32(cx, cy, cz), f32(3, cx, cy, cz)],
                chunks,
                [VMEM] * 10,
                [pltpu.VMEM((cx, FIELDS * cy, cz), jnp.float32)],
            )


def solution(mesh):
    in_specs = (
        P("gx", "gy", None),
        P(None, "gx", "gy", None),
        P(None, None, "gx", "gy", None),
        P("gx", "gy", None),
        P("gx", "gy", None),
        P("gx", "gy", None),
        P(),
    )
    out_specs = (P("gx", "gy", None), P(None, "gx", "gy", None))
    return jax.shard_map(
        on_device, mesh=mesh, in_specs=in_specs, out_specs=out_specs, check_vma=False
    )
```

```python
import functools

import jax
import jax.numpy as jnp
from jax import lax
from jax.experimental import pallas as pl
from jax.experimental.pallas import tpu as pltpu
from jax.sharding import PartitionSpec as P


STEPS = 2
BUOYANCY = 0.8
FIELDS = 4
SUB = 8
VMEM = pl.BlockSpec(memory_space=pltpu.VMEM)
SMEM = pl.BlockSpec(memory_space=pltpu.SMEM)


def call(body, outs, args, specs, scratch=(), flops=1000000):
    moved = sum(a.size for a in args) * 4 + sum(o.size for o in outs) * 4
    return pl.pallas_call(
        body,
        out_shape=tuple(outs),
        in_specs=list(specs),
        out_specs=tuple(VMEM for _ in outs),
        scratch_shapes=list(scratch),
        compiler_params=pltpu.CompilerParams(vmem_limit_bytes=8 * 1024 * 1024),
        cost_estimate=pl.CostEstimate(flops=flops, bytes_accessed=moved, transcendentals=0),
    )(*args)


def f32(*shape):
    return jax.ShapeDtypeStruct(shape, jnp.float32)


def sublane(shape):
    return lax.broadcasted_iota(jnp.int32, shape, 0)


def turn(v, steps, axis):
    return pltpu.roll(v, steps % v.shape[axis], axis)


def cubic_weights(position):
    squared = position * position
    cubed = squared * position
    return (
        (2.0 * squared - cubed - position) * 0.5,
        (3.0 * cubed - 5.0 * squared + 2.0) * 0.5,
        (4.0 * squared - 3.0 * cubed + position) * 0.5,
        (cubed - squared) * 0.5,
    )


def columns_body(cy, vel, labels, rates_at, left, right, near_vel, near_labels, rates, sem):
    copies = [pltpu.make_async_copy(rates_at, rates, sem.at[4])]
    for n, y0 in enumerate((0, cy - 2)):
        at = pl.ds(y0, 2)
        copies.append(pltpu.make_async_copy(vel.at[:, :, at, :], near_vel.at[n], sem.at[2 * n]))
        copies.append(pltpu.make_async_copy(labels.at[:, at, :], near_labels.at[n], sem.at[2 * n + 1]))
    for copy in copies:
        copy.start()
    for copy in copies:
        copy.wait()
    for n, out in enumerate((left, right)):
        for k in range(2):
            cell = jnp.where(near_labels[n, :, k, :] == 1, rates[1], rates[0])
            out[:, FIELDS * k, :] = cell
            for f in range(3):
                out[:, FIELDS * k + f + 1, :] = near_vel[n, f, :, k, :]


def in_hbm(value):
    return pltpu.with_memory_space_constraint(value, pltpu.HBM)


def prep_body(cx, cy, step, *refs):
    level_at, vel_at, labels_at, rates_at, sx_at, sy_at, fraction = refs[:7]
    state, rate, weights, own_moves = refs[7:11]
    level, vel, labels, rates, sx, sy, near, sem = refs[11:]
    copies = [
        pltpu.make_async_copy(a, b, sem.at[n])
        for n, (a, b) in enumerate(
            zip(
                (vel_at, level_at, labels_at, rates_at, sx_at, sy_at, fraction.at[step]),
                (vel, level, labels, rates, sx, sy, near),
            )
        )
    ]
    for copy in copies:
        copy.start()
    for copy in copies[:6]:
        copy.wait()
    for n in range(STEPS):
        own_moves[n] = jnp.full(own_moves.shape[1:], sx[0, 0, n].astype(jnp.float32))
        own_moves[STEPS + n] = jnp.full(own_moves.shape[1:], sy[0, 0, n].astype(jnp.float32))

    def row(x, _):
        state[x, pl.ds(0, cy, stride=FIELDS), :] = level[x]
        for f in range(3):
            state[x, pl.ds(f + 1, cy, stride=FIELDS), :] = vel[f, x]
        cell = jnp.where(labels[x] == 1, rates[1], rates[0])
        for f in range(FIELDS):
            rate[x, pl.ds(f, cy, stride=FIELDS), :] = cell
        return 0

    lax.fori_loop(0, cx, row, 0)
    copies[6].wait()
    fill_weights(cx, cy, near, weights)


def edge_rows_body(cx, pairs, mix, *refs):
    sources, (top, bot) = refs[:-2], refs[-2:]
    state, ym, yp = sources[0], sources[-2], sources[-1]
    wide = pairs + 2
    for out, rows in ((top, (0, 1)), (bot, (cx - 2, cx - 1))):
        for k, x in enumerate(rows):
            out[k * wide] = ym[x]
            out[k * wide + pairs + 1] = yp[x]
            for q in range(pairs):
                v = state[x * pairs + q]
                if mix:
                    v = jnp.where(sublane(v.shape) % FIELDS == 0, sources[1][x * pairs + q], v)
                out[k * wide + q + 1] = v


def fill_weights(cx, cy, near, out):
    pairs = cy // 2

    def row(x, _):
        for d in range(3):
            for k, w in enumerate(cubic_weights(near[d, x])):
                table = out.at[4 * d + k, pl.ds(x * pairs, pairs)].reshape(FIELDS * cy, w.shape[-1])
                for f in range(FIELDS):
                    table[pl.ds(f, cy, stride=FIELDS), :] = w
        return 0

    lax.fori_loop(0, cx, row, 0)


def weights_body(cx, cy, step, fraction, out, near, sem):
    copy = pltpu.make_async_copy(fraction.at[step], near, sem)
    copy.start()
    copy.wait()
    fill_weights(cx, cy, near, out)


def fill_rows(pad, at, rows, pairs, own, ym, yp, change):
    wide = pairs + 2
    for n, x in enumerate(rows):
        pad[(at + n) * wide] = change(ym[x])
        pad[(at + n) * wide + pairs + 1] = change(yp[x])
        for q in range(pairs):
            pad[(at + n) * wide + q + 1] = own[x * pairs + q]


def spread_rate(v):
    v = jnp.where(sublane(v.shape) % FIELDS == 0, v, 0.0)
    v = v + turn(v, 1, 0)
    return v + turn(v, 2, 0)


def same(v):
    return v


def coef_row(pad, base, ax, yu, yd, zu, zd, c0, r, wide):
    shape = pad.shape[1:]
    half = sublane(shape) < FIELDS
    scale = jnp.where(sublane(shape) % FIELDS == 0, 0.0, 0.5)
    flipped = [turn(pad[base + j], FIELDS, 0) for j in range(wide)]
    for j in range(wide):
        own = pad[base + j]
        up = jnp.where(half, flipped[j], flipped[min(j + 1, wide - 1)])
        down = jnp.where(half, flipped[max(j - 1, 0)], flipped[j])
        at = r * wide + j
        cyu = (own + up) * scale
        cyd = (own + down) * scale
        czu = (own + turn(own, -1, 1)) * scale
        czd = (own + turn(own, 1, 1)) * scale
        yu[at] = cyu
        yd[at] = cyd
        zu[at] = czu
        zd[at] = czd
        c0[at] = 1.0 - (ax[at] + ax[at + wide] + cyu + cyd + czu + czd)


def face_row(pad, base, ax, r, wide):
    scale = jnp.where(sublane(pad.shape[1:]) % FIELDS == 0, 0.0, 0.5)
    for j in range(wide):
        ax[r * wide + j] = (pad[base - wide + j] + pad[base + j]) * scale


def coef_inner_body(cx, pairs, rate, ym, yp, ax, yu, yd, zu, zd, c0, pad):
    wide = pairs + 2

    def copy(x, _):
        pad[x * wide] = spread_rate(ym[x])
        pad[x * wide + pairs + 1] = spread_rate(yp[x])
        for q in range(pairs):
            pad[x * wide + q + 1] = rate[x * pairs + q]
        return 0

    lax.fori_loop(0, cx, copy, 0)

    def faces(r, _):
        face_row(pad, (r - 1) * wide, ax, r, wide)
        return 0

    lax.fori_loop(2, cx + 1, faces, 0)

    def row(r, _):
        coef_row(pad, (r - 1) * wide, ax, yu, yd, zu, zd, c0, r, wide)
        return 0

    lax.fori_loop(2, cx, row, 0)


def coef_outer_body(cx, pairs, rate, xm, xp, ym, yp, ax_inner, *refs):
    outs, pad = refs[:6], refs[6]
    ax, yu, yd, zu, zd, c0 = outs
    wide = pairs + 2
    outer_pad(pad, cx, pairs, rate, xm, xp, ym, yp, spread_rate)
    for half_at, faces in ((0, (0, 1)), (1, (4, 5))):
        base = 4 * half_at * wide
        for n in faces:
            face_row(pad, base + (1 + n - (3 if half_at else 0)) * wide, ax, n, wide)
    for j in range(wide):
        ax[2 * wide + j] = ax_inner[2 * wide + j]
        ax[3 * wide + j] = ax_inner[cx * wide + j]
    for n in range(2):
        coef_row(pad, (1 + n) * wide, ax, yu, yd, zu, zd, c0, n, wide)
    shifted = ax.at[pl.ds(wide, 5 * wide)]
    for n in range(2):
        coef_row(pad, (5 + n) * wide, shifted, yu, yd, zu, zd, c0, 2 + n, wide)


def outer_pad(pad, cx, pairs, own, xm, xp, ym, yp, change):
    wide = pairs + 2
    for k in range(2 * wide):
        pad[k] = change(xm[k])
        pad[6 * wide + k] = change(xp[k])
    fill_rows(pad, 2, (0, 1), pairs, own, ym, yp, change)
    fill_rows(pad, 4, (cx - 2, cx - 1), pairs, own, ym, yp, change)


def sweep_row(src, base, lo, hi, coefs, at, half):
    ax, yu, yd, zu, zd, c0, wide = coefs
    own = {j: src[base + j] for j in range(max(lo - 1, 0), min(hi + 1, wide))}
    flipped = {j: turn(v, FIELDS, 0) for j, v in own.items()}
    for j in range(lo, hi):
        up = jnp.where(half, flipped[j], flipped.get(j + 1, flipped[j]))
        down = jnp.where(half, flipped.get(j - 1, flipped[j]), flipped[j])
        v = own[j]
        k = at + j
        total = c0[k] * v + ax[k] * src[base - wide + j] + ax[k + wide] * src[base + wide + j]
        total = total + yu[k] * up + yd[k] * down
        total = total + zu[k] * turn(v, -1, 1) + zd[k] * turn(v, 1, 1)
        yield j, total


def lifts(shape):
    return jnp.where(sublane(shape) % FIELDS == 0, BUOYANCY, 0.0)


def diffuse_inner(cx, pairs, own, ym, yp, coefs, pad, mid, g):
    wide = pairs + 2
    half = sublane(pad.shape[1:]) < FIELDS
    lift = lifts(pad.shape[1:])
    coefs = tuple(coefs) + (wide,)

    def copy(x, _):
        pad[x * wide] = ym[x]
        pad[x * wide + pairs + 1] = yp[x]
        for q in range(pairs):
            pad[x * wide + q + 1] = own[x * pairs + q]
        return 0

    lax.fori_loop(0, cx, copy, 0)

    def first(x, _):
        for j, v in sweep_row(pad, x * wide, 0, wide, coefs, (x + 1) * wide, half):
            mid[x * wide + j] = v
        return 0

    lax.fori_loop(1, cx - 1, first, 0)

    def second(x, _):
        for j, v in sweep_row(mid, x * wide, 1, pairs + 1, coefs, (x + 1) * wide, half):
            g[x * pairs + j - 1] = v + lift * turn(v, -3, 0)
        return 0

    lax.fori_loop(2, cx - 2, second, 0)


def diffuse_outer(cx, pairs, own, xm, xp, ym, yp, coefs, outer, mid_inner, g_inner, pad, mid, g):
    wide = pairs + 2
    shape = pad.shape[1:]
    half = sublane(shape) < FIELDS
    lift = lifts(shape)
    zero = jnp.zeros(shape, jnp.float32)
    for k in range(3 * pairs):
        g[k] = zero
        g[(cx + 3) * pairs + k] = zero

    def copy(x, _):
        for q in range(pairs):
            g[(x + 3) * pairs + q] = g_inner[x * pairs + q]
        return 0

    lax.fori_loop(2, cx - 2, copy, 0)
    outer_pad(pad, cx, pairs, own, xm, xp, ym, yp, same)
    for j in range(wide):
        mid[2 * wide + j] = mid_inner[wide + j]
        mid[3 * wide + j] = mid_inner[2 * wide + j]
        mid[4 * wide + j] = mid_inner[(cx - 3) * wide + j]
        mid[5 * wide + j] = mid_inner[(cx - 2) * wide + j]
    low = tuple(outer) + (wide,)
    high = (outer[0].at[pl.ds(wide, 5 * wide)],) + tuple(outer[1:]) + (wide,)
    for n, (src, to, table) in enumerate(((1, 0, low), (2, 1, low), (5, 6, high), (6, 7, high))):
        lo, hi = (1, pairs + 1) if n in (0, 3) else (0, wide)
        for j, v in sweep_row(pad, src * wide, lo, hi, table, n * wide, half):
            mid[to * wide + j] = v
    inner = tuple(coefs) + (wide,)
    for src, x, table, at in (
        (1, 0, low, 1),
        (2, 1, inner, 2),
        (5, cx - 2, inner, cx - 1),
        (6, cx - 1, high, 2),
    ):
        for j, v in sweep_row(mid, src * wide, 1, pairs + 1, table, at * wide, half):
            g[(x + 3) * pairs + j - 1] = v + lift * turn(v, -3, 0)


def patch_row(g, w, cx, pairs, at, lead):
    shape = g.shape[1:]
    half = sublane(shape) < FIELDS
    rows = [(at + 1 - a + lead, jnp.clip(at + 1 - a, 0, cx - 1)) for a in range(4)]
    out = []
    zero = jnp.zeros(shape, jnp.float32)

    def finish(acc0, acc1, acc1_before):
        flipped = turn(acc1, FIELDS, 0) if acc1 is not None else zero
        flipped_before = turn(acc1_before, FIELDS, 0) if acc1_before is not None else zero
        value = jnp.where(half, flipped_before, flipped)
        return value if acc0 is None else acc0 + value

    p1 = p2 = p3 = p3_old = acc1_old = None
    for q in range(pairs):
        sums = [[None] * 4 for _ in range(4)]
        for a in range(4):
            padded, row = rows[a]
            k = row * pairs + q
            h = g[padded * pairs + q] * w[a, k]
            wy = [w[4 + b, k] for b in range(4)]
            for c in range(4):
                hc = h * w[8 + c, k]
                for b in range(4):
                    t = hc * wy[b]
                    sums[b][c] = t if sums[b][c] is None else sums[b][c] + t
        p = []
        for b in range(4):
            s = sums[b]
            p.append((turn(s[0], -1, 1) + s[1]) + (turn(s[2], 1, 1) + turn(s[3], 2, 1)))
        acc1 = p[0] if p2 is None else p2 + p[0]
        acc0 = p1 if p3_old is None else p1 + p3_old
        out.append(finish(acc0, acc1, acc1_old))
        p3_old = p3
        p1, p2, p3 = p[1], p[2], p[3]
        acc1_old = acc1
    out.append(finish(p1 if p3_old is None else p1 + p3_old, p2, acc1_old))
    out.append(finish(p3, None, p2))
    return out


def spread(cx, pairs, rows_of, count, lead, g, w, moves, step, own, right, left, far):
    move_x = moves[step]
    move_y = moves[STEPS + step]
    here = jnp.where(move_y == 0, 1.0, 0.0)
    up = jnp.where(move_y == 1, 1.0, 0.0)
    down = jnp.where(move_y == -1, 1.0, 0.0)

    def row(i, _):
        out = patch_row(g, w, cx, pairs, rows_of(i), lead)
        low, high = out[0], out[pairs + 1]
        for q in range(pairs):
            v = out[q + 1]
            o, r, l = v * here, v * up, v * down
            if q == 0:
                o = o + high * down
                r = r + high * here
            if q == pairs - 1:
                o = o + low * up
                l = l + low * here
            own[i * pairs + q] = o
            right[i * pairs + q] = r
            left[i * pairs + q] = l
        far[i] = high * up + low * down
        return 0

    lax.fori_loop(0, count, row, 0)
    right[count * pairs] = move_x
    left[count * pairs] = move_x
    far[count] = move_x
    far[count + 1] = move_y


def inner_body(cx, pairs, step, rows_of, count, *refs):
    own, ym, yp, coefs, w, moves = refs[0], refs[1], refs[2], refs[3:9], refs[9], refs[10]
    o, r, l, far, mid, g, pad = refs[11:]
    diffuse_inner(cx, pairs, own, ym, yp, coefs, pad, mid, g)
    spread(cx, pairs, rows_of, count, 0, g, w, moves, step, o, r, l, far)


def outer_body(cx, pairs, step, runs, *refs):
    own, halos, coefs, outer = refs[0], refs[1:5], refs[5:11], refs[11:17]
    mid_inner, g_inner, w, moves = refs[17:21]
    outs, (pad, mid, g) = refs[21:29], refs[29:]
    diffuse_outer(cx, pairs, own, *halos, coefs, outer, mid_inner, g_inner, pad, mid, g)
    for n, (rows_of, count) in enumerate(runs):
        spread(cx, pairs, rows_of, count, 3, g, w, moves, step, *outs[4 * n : 4 * n + 4])


def gather_body(pairs, step, main, rims, *refs):
    own, right, left, far_low, far_high, own_moves = refs[:6]
    outs = refs[6:11]
    count = own.shape[0] // pairs
    skip = len(rims)
    mine = own_moves[step]
    moves = (mine, right[count * pairs], left[count * pairs])
    far_moves = (far_low[count], far_high[count])
    far_gates = (far_low[count + 1] == 1.0, far_high[count + 1] == -1.0)
    side = 2 * lax.rem(lax.axis_index("gx"), 2) - 1
    targets = (side, -side, 2 * side, -2 * side, jnp.int32(0))

    def hit(move, t):
        return jnp.where(move == t.astype(jnp.float32), 1.0, 0.0)

    def total(masks, fars, i, q):
        v = masks[0] * own[i * pairs + q] + masks[1] * right[i * pairs + q] + masks[2] * left[i * pairs + q]
        if q == 0:
            v = v + fars[0] * far_low[i]
        if q == pairs - 1:
            v = v + fars[1] * far_high[i]
        return v

    def masks_of(t):
        masks = [hit(m, t) for m in moves]
        fars = [jnp.where(gate, hit(m, t), 0.0) for gate, m in zip(far_gates, far_moves)]
        return masks, fars

    for out, t in zip(outs, targets):
        masks, fars = masks_of(t)

        def row(i, _, out=out, masks=masks, fars=fars):
            for q in range(pairs):
                out[i * pairs + q] = total(masks, fars, i + skip, q)
            return 0

        lax.fori_loop(0, main, row, 0)
        for source, (row_at, step_to) in enumerate(rims):
            masks, fars = masks_of(t + step_to)
            for q in range(pairs):
                out[row_at * pairs + q] = out[row_at * pairs + q] + total(masks, fars, source, q)
    for source, (_, step_to) in enumerate(rims):
        masks, fars = masks_of(jnp.int32(-2 * step_to))
        for q in range(pairs):
            refs[11][source * pairs + q] = total(masks, fars, source, q)


def add_body(a, b, out):
    group = 8 if out.shape[0] % 8 == 0 else 1

    def rows(i, _):
        for j in range(group):
            out[i * group + j] = a[i * group + j] + b[i * group + j]
        return 0

    lax.fori_loop(0, out.shape[0] // group, rows, 0)


def merge(cx, pairs, chunks, parts, put):
    for runs, (t0, e0, f, d) in zip(chunks, (parts[0:4], parts[4:8], parts[8:12])):
        for local, base, rows in runs:

            def row(i, _, t0=t0, e0=e0, f=f, d=d, local=local, base=base):
                for q in range(pairs):
                    at = (i + local) * pairs + q
                    put(i + base, q, (t0[at] + e0[at]) + (f[at] + d[at]), False)
                return 0

            lax.fori_loop(0, rows, row, 0)
    high, low = parts[12:14]
    for q in range(pairs):
        for k in range(2):
            put(k, q, high[k * pairs + q], True)
        put(cx - 1, q, low[q], True)


def merge_body(cx, pairs, chunks, *refs):
    parts = refs[:14]
    out, left, right = refs[14:]

    def put(x, q, v, add):
        at = x * pairs + q
        out[at] = out[at] + v if add else v

    merge(cx, pairs, chunks, parts, put)
    for x in range(cx):
        left[x] = out[x * pairs]
        right[x] = out[x * pairs + pairs - 1]


def finish_body(cx, cy, pairs, chunks, *refs):
    parts = refs[:14]
    level, vel, out = refs[14:]

    def put(x, q, v, add):
        at = pl.ds(SUB * q, SUB)
        out[x, at, :] = out[x, at, :] + v if add else v

    merge(cx, pairs, chunks, parts, put)

    def row(x, _):
        level[x] = out[x, pl.ds(0, cy, stride=FIELDS), :]
        for f in range(3):
            vel[f, x] = out[x, pl.ds(f + 1, cy, stride=FIELDS), :]
        return 0

    lax.fori_loop(0, cx, row, 0)


def moved(value, axis, steps):
    count = lax.axis_size(axis)
    return lax.ppermute(value, axis, [(i, (i + steps) % count) for i in range(count)])


def swapped(value):
    return lax.ppermute(value, "gx", [(i, i ^ 1) for i in range(lax.axis_size("gx"))])


def crossed(value, sign):
    count = lax.axis_size("gx")
    return lax.ppermute(
        value, "gx", [(i, (i + (2 if i % 2 else -2) * sign) % count) for i in range(count)]
    )


def on_device(level, vel, fraction, shift_x, shift_y, labels, rates):
    cx, cy, cz = level.shape
    pairs = cy // 2
    wide = pairs + 2
    ny = lax.axis_size("gy")

    def plane(n):
        return f32(n, SUB, cz)

    def scratch(n):
        return pltpu.VMEM((n, SUB, cz), jnp.float32)

    level, vel, labels, rates = map(in_hbm, (level, vel, labels, rates))
    fraction, shift_x, shift_y = map(in_hbm, (fraction, shift_x, shift_y))
    hbm = pl.BlockSpec(memory_space=pltpu.HBM)
    rates_here = pltpu.SMEM(rates.shape, rates.dtype)
    near = pltpu.VMEM(fraction.shape[1:], fraction.dtype)
    left, right = call(
        functools.partial(columns_body, cy),
        [plane(cx)] * 2,
        (vel, labels, rates),
        [hbm] * 3,
        [
            pltpu.VMEM((2, *vel.shape[:2], 2, cz), vel.dtype),
            pltpu.VMEM((2, cx, 2, cz), labels.dtype),
            rates_here,
            pltpu.SemaphoreType.DMA((5,)),
        ],
    )
    last = STEPS - 1
    table = f32(12, cx * pairs + 1, SUB, cz)
    state, rate, weights_last, own_moves = call(
        functools.partial(prep_body, cx, cy, last),
        [f32(cx, FIELDS * cy, cz)] * 2 + [table, plane(2 * STEPS)],
        (level, vel, labels, rates, shift_x, shift_y, fraction),
        [hbm] * 7,
        [pltpu.VMEM(a.shape, a.dtype) for a in (level, vel, labels)]
        + [pltpu.SMEM(a.shape, a.dtype) for a in (rates, shift_x, shift_y)]
        + [near, pltpu.SemaphoreType.DMA((7,))],
    )
    state = state.reshape(cx * pairs, SUB, cz)
    rate = rate.reshape(cx * pairs, SUB, cz)
    weights = [
        call(
            functools.partial(weights_body, cx, cy, s),
            [table],
            (fraction,),
            [hbm],
            [near, pltpu.SemaphoreType.DMA],
        )[0]
        for s in range(last)
    ] + [weights_last]
    coefs = outer = None

    inner = 4
    count_a = cx - 2 * inner + 1
    behind = inner + count_a
    main = (count_a, inner, cx - behind)
    chunk_runs = (((0, inner, main[0]),), ((0, 0, main[1]),), ((0, behind, main[2]),))

    def rows_a(i):
        return i + inner

    def rows_b(i):
        return jnp.where(i < 2, cx + i, i - 2)

    def rows_c(i):
        return jnp.where(i < 1, -1, i - 1 + behind)

    counts = (main[0], main[1] + 2, main[2] + 1)
    rims_of = ((), ((0, -1), (1, -1)), ((main[2] - 1, 1),))

    def outs(n):
        return [plane(n * pairs), plane(n * pairs + 1), plane(n * pairs + 1), plane(n + 2)]

    for step in range(STEPS - 1, -1, -1):
        first = coefs is None
        ym = moved(right, "gy", 1)
        yp = moved(left, "gy", -1)
        states = (state, rate) if first else (state,)
        top, bot = call(
            functools.partial(edge_rows_body, cx, pairs, first),
            [plane(2 * wide)] * 2,
            (*states, ym, yp),
            [VMEM] * (len(states) + 2),
        )
        xm = moved(bot, "gx", 1)
        xp = moved(top, "gx", -1)
        if first:
            coefs = call(
                functools.partial(coef_inner_body, cx, pairs),
                [plane((cx + 3) * wide)] + [plane((cx + 2) * wide)] * 5,
                (rate, ym, yp),
                [VMEM] * 3,
                [scratch(cx * wide)],
            )
        *sent_a, mid, g = call(
            functools.partial(inner_body, cx, pairs, step, rows_a, counts[0]),
            outs(counts[0]) + [plane(cx * wide), plane(cx * pairs)],
            (state, ym, yp, *coefs, weights[step], own_moves),
            [VMEM] * 11,
            [scratch(cx * wide)],
            flops=20000000,
        )
        if first:
            outer = call(
                functools.partial(coef_outer_body, cx, pairs),
                [plane(6 * wide)] + [plane(4 * wide)] * 5,
                (rate, xm, xp, ym, yp, coefs[0]),
                [VMEM] * 6,
                [scratch(8 * wide)],
            )
        sent_b = call(
            functools.partial(outer_body, cx, pairs, step, ((rows_b, counts[1]), (rows_c, counts[2]))),
            outs(counts[1]) + outs(counts[2]),
            (state, xm, xp, ym, yp, *coefs, *outer, mid, g, weights[step], own_moves),
            [VMEM] * 21,
            [scratch(8 * wide), scratch(8 * wide), scratch((cx + 6) * pairs)],
            flops=10000000,
        )
        chunks, rims = [], []
        for n, (own, right, left, far) in enumerate((sent_a, sent_b[:4], sent_b[4:])):
            if n:
                own, _ = lax.optimization_barrier((own, chunks[-4]))
            right = moved(right, "gy", 1)
            left = moved(left, "gy", -1)
            far_low = moved(far, "gy", 2)
            far_high = far_low if ny == 4 else moved(far, "gy", -2)
            e1, e0, f, k, t0, *rim = call(
                functools.partial(gather_body, pairs, step, main[n], rims_of[n]),
                [plane(main[n] * pairs)] * 5 + ([plane(len(rims_of[n]) * pairs)] if n else []),
                (own, right, left, far_low, far_high, own_moves),
                [VMEM] * 6,
                flops=3000000,
            )
            e1 = swapped(e1)
            f = crossed(f, 1)
            e0 = swapped(e0)
            (d,) = call(add_body, [plane(main[n] * pairs)], (k, e1), [VMEM] * 2)
            d = crossed(d, -1)
            chunks += [t0, e0, f, d]
            rims += rim
        high, low = rims
        high = moved(high, "gx", 3)
        low = moved(low, "gx", -3)
        chunks += [high, low]
        if step:
            state, left, right = call(
                functools.partial(merge_body, cx, pairs, chunk_runs),
                [plane(cx * pairs)] + [plane(cx)] * 2,
                chunks,
                [VMEM] * 14,
            )
        else:
            return call(
                functools.partial(finish_body, cx, cy, pairs, chunk_runs),
                [f32(cx, cy, cz), f32(3, cx, cy, cz)],
                chunks,
                [VMEM] * 14,
                [pltpu.VMEM((cx, FIELDS * cy, cz), jnp.float32)],
            )


def solution(mesh):
    in_specs = (
        P("gx", "gy", None),
        P(None, "gx", "gy", None),
        P(None, None, "gx", "gy", None),
        P("gx", "gy", None),
        P("gx", "gy", None),
        P("gx", "gy", None),
        P(),
    )
    out_specs = (P("gx", "gy", None), P(None, "gx", "gy", None))
    return jax.shard_map(
        on_device, mesh=mesh, in_specs=in_specs, out_specs=out_specs, check_vma=False
    )
```
